128 devices in a mesh: dp: 32 (over y, z, core), fsdp: 4 (over x).
Axes of the slice: x: 4, y: 4, z: 4, core: 2. Of those that a mesh axis runs over, the one named last changes fastest.
Arguments:
- tokens: bfloat16 [65536, 4096], P(('dp', 'fsdp')), may hold values from -0.75 to 0.75
- doc_ids: int32 [65536], P(('dp', 'fsdp')), may hold values from 0 to 63, never falling along the last dimension, each value on 1 to 2048 neighbouring positions
- attn_gain: float32 [4096], replicated, may hold values from 0.1 to 1.9
- mlp_gain: float32 [4096], replicated, may hold values from 0.1 to 1.9
- w_query: bfloat16 [4096, 512], P(('dp', 'fsdp')), may hold values from -1 to 1
- w_key_value: bfloat16 [4096, 256], P(('dp', 'fsdp')), may hold values from -3 to 3
- w_out: bfloat16 [512, 4096], P(None, ('dp', 'fsdp')), may hold values from -0.25 to 0.25
- w_gate: bfloat16 [4096, 1024], P(('dp', 'fsdp')), may hold values from -0.09375 to 0.09375
- w_up: bfloat16 [4096, 1024], P(('dp', 'fsdp')), may hold values from -0.09375 to 0.09375
- w_down: bfloat16 [1024, 4096], P(None, ('dp', 'fsdp')), may hold values from -0.1875 to 0.1875
Outputs:
- mixed: bfloat16 [65536, 4096], P(('dp', 'fsdp'))
The draws below stay inside these ranges and needn't reach their ends.
Inputs may be any that keep to these rules, and one draw needn't show every extreme that they name: `doc_ids`: document numbers never fall along the pack, and every document has at most 2048 tokens.
All inputs are finite; a program needn't handle non-finite values.
Results may differ from the reference program's by a relative error of at most 0.02.
The reference program's roundings to bfloat16 on the way count: a program that leaves them out, or rounds other values in their place, can miss the bound.
Values may be sent and summed in bfloat16 or wider, within the bound.
No kernel may reach another device: no remote copies, remote signals or barrier semaphores. Data moves between devices by JAX's collectives and lax.ppermute only.
A program may use at most 128 MiB of HBM per device.

```python
import math
import jax
import jax.numpy as jnp
import numpy as np
from jax import lax

D = 4096
HQ = 4
HD = 128
FF = 1024
TOK_DEV = 512
HALO = 2048
TOKENS = 65536
DOCS = 64
N_DP = 32
N_FSDP = 4


def shared_query(key):
    base = jax.random.normal(jax.random.fold_in(key, 11), (D, HQ * HD), jnp.float32)
    return jnp.clip(base, -6.0, 6.0) / math.sqrt(D)


def draw_w_query(key, part):
    return shared_query(key).astype(jnp.bfloat16)


def draw_w_key_value(key, part):
    fresh = jax.random.normal(jax.random.fold_in(key, 23), (D, 2 * HD), jnp.float32)
    fresh = jnp.clip(fresh, -6.0, 6.0) / math.sqrt(D)
    return fresh.astype(jnp.bfloat16)


def block_levels(stream_key, extent, split, smallest, high):
    def one(dim, parts):
        steps = jax.random.uniform(jax.random.fold_in(jax.random.fold_in(stream_key, 6), dim), (parts,), jnp.float32, smallest / len(split), high / len(split))
        return jnp.repeat(jnp.exp(steps), extent[dim] // parts).reshape((-1,) + (1,) * (len(extent) - dim - 1))

    level = one(*split[0])
    for cut in split[1:]:
        level = level * one(*cut)
    return level


def split_up(count, total, most, slope):
    weights = [(1 << 20) // math.isqrt(grade ** slope) + 1 for grade in range(2, count + 1)]
    rest, holding = total - most - (count - 1), [1] * (count - 1)
    while rest > 0:
        movable = [i for i in range(count - 1) if holding[i] < most]
        whole, remaining = sum([weights[i] for i in movable]), rest
        for i in movable:
            addition = min(most - holding[i], max(1, remaining * weights[i] // whole), rest)
            holding[i] = holding[i] + addition
            rest = rest - addition
    return np.array([most] + holding)


def ragged_sizes(own_key, number_of, total, most, skew):
    if number_of == 2:
        one = jax.random.randint(own_key, (), max(1, total - most), min(most, total - 1) + 1)
        return jnp.stack([one, total - one])
    sizes = jnp.asarray(split_up(number_of, total, most, skew), jnp.int32)
    pairs = (number_of - 1) // 2
    donor, receiver = sizes[1:1 + 2 * pairs:2], sizes[2:2 + 2 * pairs:2]
    margin = jnp.minimum(donor - 1, most - receiver)
    passed = jax.random.randint(jax.random.fold_in(own_key, 1), (pairs,), 0, 1 << 20) % (margin + 1)
    sizes = sizes.at[1:1 + 2 * pairs:2].set(donor - passed).at[2:2 + 2 * pairs:2].set(receiver + passed)
    return sizes[jax.random.permutation(jax.random.fold_in(own_key, 2), number_of)]


def noise(stream_key, extent, spread, limit, shards=(), kind=jnp.bfloat16):
    values = spread * jax.random.normal(stream_key, extent, jnp.float32)
    if shards:
        values = values * block_levels(stream_key, extent, shards, -0.22, 0.18)
    return jnp.clip(values, -limit, limit).astype(kind)


def setup_inputs(seed: int = 0) -> dict:
    splits = jax.random.split(jax.random.key(seed), 11)
    return {
        "tokens": noise(splits[0], (TOKENS, D), 0.05, 0.75, ((0, 128),)),
        "doc_ids": jnp.searchsorted(jnp.cumsum(ragged_sizes(splits[1], DOCS, TOKENS, HALO, 1)), jnp.arange(TOKENS), side="right").astype(jnp.int32),
        "attn_gain": jnp.clip(1.0 + 0.18 * jax.random.normal(splits[2], (D,), jnp.float32), 0.1, 1.9),
        "mlp_gain": jnp.clip(1.0 + 0.18 * jax.random.normal(splits[3], (D,), jnp.float32), 0.1, 1.9),
        "w_query": draw_w_query(jax.random.fold_in(splits[10], 71), 0),
        "w_key_value": draw_w_key_value(jax.random.fold_in(splits[10], 71), 0),
        "w_out": noise(splits[6], (HQ * HD, D), (HQ * HD) ** -0.5, 0.25, ((1, 128),)),
        "w_gate": noise(splits[7], (D, FF), D ** -0.5, 0.09375, ((0, 128),)),
        "w_up": noise(splits[8], (D, FF), D ** -0.5, 0.09375, ((0, 128),)),
        "w_down": noise(splits[9], (FF, D), FF ** -0.5, 0.1875, ((1, 128),)),
    }


EPS = 1e-05
THETA = 500000.0
NEGATIVE = -1e+30

def rms_scale(values, gain):
    wide = values.astype(jnp.float32)
    power = lax.optimization_barrier(jnp.mean(wide * wide, axis=-1, keepdims=True))
    return (wide * lax.rsqrt(power + EPS) * gain).astype(jnp.bfloat16)

def rotate(values, position):
    head = values.shape[-1]
    half = head // 2
    freqs = THETA ** (-2.0 * jnp.arange(half, dtype=jnp.float32) / head)
    angle = position.astype(jnp.float32)[:, None, None] * freqs[None, None, :]
    cosine = jnp.cos(angle)
    sine = jnp.sin(angle)
    first = values[..., :half]
    second = values[..., half:]
    return jnp.concatenate([first * cosine - second * sine, second * cosine + first * sine], axis=-1)

def widen(values):
    return lax.optimization_barrier(values).astype(jnp.float32)

def attend(query, keys, values, key_marks, marks, offset):
    scores = jnp.einsum('qhd,kd->hqk', widen(query), widen(keys)) / math.sqrt(query.shape[-1])
    key_index = jnp.arange(keys.shape[0], dtype=jnp.int32)
    query_index = jnp.arange(query.shape[0], dtype=jnp.int32) + offset
    allowed = (key_marks[None, :] == marks[:, None]) & (key_index[None, :] <= query_index[:, None])
    scores = jnp.where(allowed[None, :, :], scores, NEGATIVE)
    peak = lax.optimization_barrier(jnp.max(scores, axis=2, keepdims=True))
    weights = jnp.exp(scores - peak)
    totals = lax.optimization_barrier(jnp.sum(weights, axis=2))
    mixed = jnp.einsum('hqk,kd->qhd', widen(weights.astype(jnp.bfloat16)), widen(values))
    return mixed / jnp.transpose(totals)[:, :, None]

def reference(tokens, doc_ids, attn_gain, mlp_gain, w_query, w_key_value, w_out, w_gate, w_up, w_down):
    total_rows = tokens.shape[0]
    normed = rms_scale(tokens, attn_gain)
    query_raw = jnp.dot(normed, w_query, preferred_element_type=jnp.float32)
    pair_raw = jnp.dot(normed, w_key_value, preferred_element_type=jnp.float32)
    position = jnp.arange(total_rows, dtype=jnp.int32)
    query = rotate(query_raw.reshape(total_rows, HQ, HD), position).astype(jnp.bfloat16)
    keys = rotate(pair_raw[:, None, :HD], position)[:, 0, :].astype(jnp.bfloat16)
    values = pair_raw[:, HD:].astype(jnp.bfloat16)
    marks = doc_ids + 1
    key_padded = jnp.concatenate([jnp.zeros((HALO, HD), jnp.bfloat16), keys], axis=0)
    value_padded = jnp.concatenate([jnp.zeros((HALO, HD), jnp.bfloat16), values], axis=0)
    mark_padded = jnp.concatenate([jnp.zeros((HALO,), jnp.int32), marks], axis=0)

    def one_rank(rank):
        start = (rank * TOK_DEV).astype(jnp.int32)
        rank_query = lax.dynamic_slice_in_dim(query, start, TOK_DEV, 0)
        rank_marks = lax.dynamic_slice_in_dim(marks, start, TOK_DEV, 0)
        rank_keys = lax.dynamic_slice_in_dim(key_padded, start, HALO + TOK_DEV, 0)
        rank_values = lax.dynamic_slice_in_dim(value_padded, start, HALO + TOK_DEV, 0)
        key_marks = lax.dynamic_slice_in_dim(mark_padded, start, HALO + TOK_DEV, 0)
        mixed = attend(rank_query, rank_keys, rank_values, key_marks, rank_marks, HALO)
        return mixed.reshape(TOK_DEV, HQ * HD).astype(jnp.bfloat16)
    attended = lax.map(one_rank, jnp.arange(N_DP * N_FSDP, dtype=jnp.int32)).reshape(total_rows, HQ * HD)
    projected = jnp.dot(attended, w_out, preferred_element_type=jnp.float32)
    resid = (tokens.astype(jnp.float32) + projected).astype(jnp.bfloat16)
    resid = lax.optimization_barrier(resid)
    normed_mlp = rms_scale(resid, mlp_gain)
    gate = jnp.dot(normed_mlp, w_gate, preferred_element_type=jnp.float32)
    up_value = jnp.dot(normed_mlp, w_up, preferred_element_type=jnp.float32)
    hidden = (jax.nn.silu(gate) * up_value).astype(jnp.bfloat16)
    down = jnp.dot(hidden, w_down, preferred_element_type=jnp.float32)
    return (resid.astype(jnp.float32) + down).astype(jnp.bfloat16)
```

```python
import math

import jax
import jax.numpy as jnp
from jax import lax
from jax.sharding import Mesh
from jax.sharding import PartitionSpec as P

SPAN = 4


EPS = 1e-05
THETA = 500000.0
NEGATIVE = -1e30
RANKS = ("y", "z", "core", "x")
CHIPS = ("y", "z", "x")


def shifted(array, axis, by):
    length = lax.axis_size(axis)
    pairs = [(i, i + by) for i in range(length) if 0 <= i + by < length]
    return lax.ppermute(array, axis, pairs)


def rms_scale(values, gain):
    wide = values.astype(jnp.float32)
    power = jnp.mean(wide * wide, axis=-1, keepdims=True)
    return (wide * lax.rsqrt(power + EPS) * gain).astype(jnp.bfloat16)


def rotate(values, position):
    head = values.shape[-1]
    half = head // 2
    freqs = THETA ** (-2.0 * jnp.arange(half, dtype=jnp.float32) / head)
    angle = position.astype(jnp.float32)[:, None, None] * freqs[None, None, :]
    cosine = jnp.cos(angle)
    sine = jnp.sin(angle)
    first = values[..., :half]
    second = values[..., half:]
    return jnp.concatenate(
        [first * cosine - second * sine, second * cosine + first * sine], axis=-1
    )


def head_scores(query, keys):
    return jnp.einsum("qhd,kd->hqk", query, keys, preferred_element_type=jnp.float32) / math.sqrt(
        query.shape[-1]
    )


def weigh_values(weights, values):
    return jnp.einsum(
        "hqk,kd->qhd", weights.astype(jnp.bfloat16), values, preferred_element_type=jnp.float32
    )


def attend_live(query, halo_pairs, halo_marks, own_pairs, marks, block):
    head = query.shape[-1]
    index = jnp.arange(query.shape[0], dtype=jnp.int32)
    allowed = (marks[None, :] == marks[:, None]) & (index[None, :] <= index[:, None])
    own_scores = jnp.where(allowed[None, :, :], head_scores(query, own_pairs[:, :head]), NEGATIVE)
    count = halo_marks.shape[0] // block
    live = jnp.sum(jnp.any(halo_marks.reshape(count, block) == marks[0], axis=1).astype(jnp.int32))
    peak = jnp.max(own_scores, axis=2)
    weights = jnp.exp(own_scores - peak[:, :, None])
    totals = jnp.sum(weights, axis=2)
    mixed = weigh_values(weights, own_pairs[:, head:])

    def add_block(step, carry):
        old_peak, old_totals, old_mixed = carry
        begin = (count - 1 - step) * block
        pairs = lax.dynamic_slice_in_dim(halo_pairs, begin, block, 0)
        block_marks = lax.dynamic_slice_in_dim(halo_marks, begin, block, 0)
        same = (block_marks[None, :] == marks[:, None])[None, :, :]
        scores = jnp.where(same, head_scores(query, pairs[:, :head]), NEGATIVE)
        new_peak = jnp.maximum(old_peak, jnp.max(scores, axis=2))
        factor = jnp.exp(old_peak - new_peak)
        block_weights = jnp.exp(scores - new_peak[:, :, None])
        new_totals = old_totals * factor + jnp.sum(block_weights, axis=2)
        new_mixed = old_mixed * jnp.transpose(factor)[:, :, None] + weigh_values(
            block_weights, pairs[:, head:]
        )
        return (new_peak, new_totals, new_mixed)

    peak, totals, mixed = lax.fori_loop(0, live, add_block, (peak, totals, mixed))
    return mixed / jnp.transpose(totals)[:, :, None]


def projection_weights(w_query, w_key_value):
    both = jnp.concatenate([w_query, w_key_value], axis=1)
    rows, width = both.shape
    chips = lax.axis_size(CHIPS)
    copies = lax.optimization_barrier(jnp.broadcast_to(both[None], (chips, rows, width)))
    own = lax.all_to_all(copies, CHIPS, 0, 0, tiled=True)
    other = lax.ppermute(own, "core", [(0, 1), (1, 0)])
    inner = lax.axis_size("x") * rows
    own = own.reshape(-1, 1, inner, width)
    other = other.reshape(-1, 1, inner, width)
    first = lax.axis_index("core") == 0
    return jnp.concatenate(
        [jnp.where(first, own, other), jnp.where(first, other, own)], axis=1
    ).reshape(-1, width)


def per_device(
    tokens, doc_ids, attn_gain, mlp_gain, w_query, w_key_value, w_out, w_gate, w_up, w_down
):
    rows = tokens.shape[0]
    rank = lax.axis_index(RANKS)
    hidden_width = w_gate.shape[1]
    rest = jnp.concatenate([w_gate, w_up, w_out.T, w_down.T], axis=1)
    rest = lax.all_gather(rest, RANKS, axis=0, tiled=True)

    normed = rms_scale(tokens, attn_gain)
    query_width = w_query.shape[1]
    pair_width = w_key_value.shape[1]
    head = pair_width // 2
    heads = query_width // head
    w_project = projection_weights(w_query, w_key_value)
    raw = jnp.dot(normed, w_project, preferred_element_type=jnp.float32)
    query_raw = raw[:, :query_width]
    pair_raw = raw[:, query_width:]
    position = rank * rows + jnp.arange(rows, dtype=jnp.int32)
    query = rotate(query_raw.reshape(rows, heads, head), position).astype(jnp.bfloat16)
    keys = rotate(pair_raw[:, None, :head], position)[:, 0, :].astype(jnp.bfloat16)
    values = pair_raw[:, head:].astype(jnp.bfloat16)
    own_pairs = jnp.concatenate([keys, values], axis=1)
    marks = doc_ids + 1
    mark_rows = marks.astype(jnp.bfloat16).reshape(-1, pair_width)
    sent = jnp.concatenate([own_pairs, mark_rows], axis=0)
    pair_pieces = []
    mark_pieces = []
    for distance in range(SPAN, 0, -1):
        moved = shifted(sent, RANKS, distance)
        pair_pieces.append(moved[:rows])
        mark_pieces.append(moved[rows:].reshape(-1).astype(jnp.int32))
    halo_pairs = jnp.concatenate(pair_pieces, axis=0)
    halo_marks = jnp.concatenate(mark_pieces, axis=0)
    mixed = attend_live(query, halo_pairs, halo_marks, own_pairs, marks, rows)
    attended = mixed.reshape(rows, query_width).astype(jnp.bfloat16)
    g, u, o = hidden_width, 2 * hidden_width, 2 * hidden_width + query_width
    projected = lax.dot_general(
        attended, rest[:, u:o], (((1,), (1,)), ((), ())), preferred_element_type=jnp.float32
    )
    resid = (tokens.astype(jnp.float32) + projected).astype(jnp.bfloat16)
    resid = lax.optimization_barrier(resid)
    normed_mlp = rms_scale(resid, mlp_gain)
    gate = jnp.dot(normed_mlp, rest[:, :g], preferred_element_type=jnp.float32)
    up_value = jnp.dot(normed_mlp, rest[:, g:u], preferred_element_type=jnp.float32)
    hidden = (jax.nn.silu(gate) * up_value).astype(jnp.bfloat16)
    down = lax.dot_general(
        hidden, rest[:, o:], (((1,), (1,)), ((), ())), preferred_element_type=jnp.float32
    )
    return (resid.astype(jnp.float32) + down).astype(jnp.bfloat16)


def solution(mesh):
    chips = Mesh(mesh.devices.reshape(4, 4, 2, 4), RANKS)
    in_specs = (
        P(RANKS, None),
        P(RANKS),
        P(),
        P(),
        P(RANKS, None),
        P(RANKS, None),
        P(None, RANKS),
        P(RANKS, None),
        P(RANKS, None),
        P(None, RANKS),
    )
    out_specs = P(RANKS, None)
    return jax.shard_map(
        per_device, mesh=chips, in_specs=in_specs, out_specs=out_specs, check_vma=False
    )
```

```python
import functools
import math

import jax
import jax.numpy as jnp
from jax import lax
from jax.experimental import pallas as pl
from jax.experimental.pallas import tpu as pltpu
from jax.sharding import Mesh
from jax.sharding import PartitionSpec as P

SPAN = 4


EPS = 1e-05
THETA = 500000.0
NEGATIVE = -1e30
RANKS = ("y", "z", "core", "x")
RING = 4
DELTAS = (0, -1, 1, 2)
MARK_ROWS = 16
SILU_BLOCK = 256


def shifted(array, axis, by):
    length = lax.axis_size(axis)
    pairs = [(i, i + by) for i in range(length) if 0 <= i + by < length]
    return lax.ppermute(array, axis, pairs)


def turned(array, axis, by):
    return lax.ppermute(array, axis, [(i, (i + by) % RING) for i in range(RING)])


def swapped(array):
    return lax.ppermute(array, "core", [(0, 1), (1, 0)])


def rms_scale(values, gain):
    wide = values.astype(jnp.float32)
    power = jnp.mean(wide * wide, axis=-1, keepdims=True)
    return (wide * lax.rsqrt(power + EPS) * gain).astype(jnp.bfloat16)


def head_scores(query, keys):
    return jnp.einsum("qhd,kd->hqk", query, keys, preferred_element_type=jnp.float32) / math.sqrt(
        query.shape[-1]
    )


def weigh_values(weights, values):
    return jnp.einsum(
        "hqk,kd->qhd", weights.astype(jnp.bfloat16), values, preferred_element_type=jnp.float32
    )


def attend_live(query, halo_pairs, halo_marks, own_pairs, marks, block):
    head = query.shape[-1]
    index = jnp.arange(query.shape[0], dtype=jnp.int32)
    allowed = (marks[None, :] == marks[:, None]) & (index[None, :] <= index[:, None])
    own_scores = jnp.where(allowed[None, :, :], head_scores(query, own_pairs[:, :head]), NEGATIVE)
    count = halo_marks.shape[0] // block
    live = jnp.sum(jnp.any(halo_marks.reshape(count, block) == marks[0], axis=1).astype(jnp.int32))
    peak = jnp.max(own_scores, axis=2)
    weights = jnp.exp(own_scores - peak[:, :, None])
    totals = jnp.sum(weights, axis=2)
    mixed = weigh_values(weights, own_pairs[:, head:])

    def add_block(step, carry):
        old_peak, old_totals, old_mixed = carry
        begin = (count - 1 - step) * block
        pairs = lax.dynamic_slice_in_dim(halo_pairs, begin, block, 0)
        block_marks = lax.dynamic_slice_in_dim(halo_marks, begin, block, 0)
        same = (block_marks[None, :] == marks[:, None])[None, :, :]
        scores = jnp.where(same, head_scores(query, pairs[:, :head]), NEGATIVE)
        new_peak = jnp.maximum(old_peak, jnp.max(scores, axis=2))
        factor = jnp.exp(old_peak - new_peak)
        block_weights = jnp.exp(scores - new_peak[:, :, None])
        new_totals = old_totals * factor + jnp.sum(block_weights, axis=2)
        new_mixed = old_mixed * jnp.transpose(factor)[:, :, None] + weigh_values(
            block_weights, pairs[:, head:]
        )
        return (new_peak, new_totals, new_mixed)

    peak, totals, mixed = lax.fori_loop(0, live, add_block, (peak, totals, mixed))
    return mixed / jnp.transpose(totals)[:, :, None]


def gathered_near(block, axis):
    return jnp.concatenate([block] + [turned(block, axis, -d) for d in DELTAS[1:]], axis=0)


def gathered_pieces(shard):
    block = gathered_near(gathered_near(shard, "x"), "y")
    half = block.shape[0] // 2
    low = turned(block, "z", 1)
    high = turned(block, "z", -1)
    far_low = turned(low[:half], "z", 1)
    far_high = turned(high[half:], "z", -1)
    pieces = (block, low, high, far_low, far_high)
    return pieces + tuple(swapped(piece) for piece in pieces)


def load_pieces(coords, pieces, target, sem, unit):
    x, y, z, core = (coords[k] for k in range(4))
    count = len(pieces) // 2
    for swap in range(2):
        block, low, high, far_low, far_high = pieces[swap * count : (swap + 1) * count]
        owner = lax.rem(core + swap, 2)
        for pz in range(RING):
            from_z = lax.rem(z + DELTAS[pz] + RING, RING)
            for py in range(RING):
                from_y = lax.rem(y + DELTAS[py] + RING, RING)
                for px in range(RING):
                    from_x = lax.rem(x + DELTAS[px] + RING, RING)
                    rank = ((from_y * RING + from_z) * 2 + owner) * RING + from_x
                    place = py * RING + px
                    if pz < 3:
                        source = (block, low, high)[pz]
                    else:
                        source = far_low if place < 8 else far_high
                        place = place % 8
                    pltpu.make_async_copy(
                        source.at[pl.ds(place * unit, unit)],
                        target.at[pl.ds(pl.multiple_of(rank * unit, unit), unit)],
                        sem,
                    ).start()


def project_kernel(head, unit, *refs):
    coords, normed, cosine, sine, mark_rows = refs[:5]
    pieces = refs[5:15]
    query, pairs, weights, sem = refs[15:]
    load_pieces(coords, pieces, weights, sem, unit)
    rows = normed.shape[0]
    width = query.shape[1]
    pltpu.make_async_copy(weights, weights, sem).wait()

    def rotated(raw):
        return raw * cosine[...] + pltpu.roll(raw, head // 2, 1) * sine[...]

    pair_raw = jnp.dot(normed[...], weights[:, width:], preferred_element_type=jnp.float32)
    pairs[:rows, :head] = rotated(pair_raw[:, :head]).astype(jnp.bfloat16)
    pairs[:rows, head:] = pair_raw[:, head:].astype(jnp.bfloat16)
    pairs[rows:, :] = mark_rows[...]
    for begin in range(0, width, 2 * head):
        raw = jnp.dot(
            normed[...], weights[:, begin : begin + 2 * head], preferred_element_type=jnp.float32
        )
        for part in range(2):
            query[:, begin + part * head : begin + (part + 1) * head] = rotated(
                raw[:, part * head : (part + 1) * head]
            ).astype(jnp.bfloat16)


def project(coords, normed, cosine, sine, mark_rows, pieces, unit, query_width, pair_width):
    rows, depth = normed.shape
    vmem = pl.BlockSpec(memory_space=pltpu.VMEM)
    hbm = pl.BlockSpec(memory_space=pl.ANY)
    return pl.pallas_call(
        functools.partial(project_kernel, pair_width // 2, unit),
        out_shape=(
            jax.ShapeDtypeStruct((rows, query_width), jnp.bfloat16),
            jax.ShapeDtypeStruct((rows + MARK_ROWS, pair_width), jnp.bfloat16),
        ),
        in_specs=[pl.BlockSpec(memory_space=pltpu.SMEM)] + [vmem] * 4 + [hbm] * len(pieces),
        out_specs=(vmem, vmem),
        scratch_shapes=[
            pltpu.VMEM((depth, query_width + pair_width), jnp.bfloat16),
            pltpu.SemaphoreType.DMA,
        ],
        compiler_params=pltpu.CompilerParams(vmem_limit_bytes=40 << 20),
        cost_estimate=pl.CostEstimate(
            flops=2 * rows * depth * (query_width + pair_width),
            bytes_accessed=2 * depth * (query_width + pair_width),
            transcendentals=0,
        ),
        name="project",
    )(coords, normed, cosine, sine, mark_rows, *pieces)


def mlp_kernel(
    attended, gain, tokens, rest, mixed,
    held, gates, outs, downs, resid, normed, hidden, squares, staged,
    out_sem, token_sem, gate_sems, down_sem, stage_sems,
):
    rows, depth = tokens.shape
    key_width = attended.shape[1]
    ff = hidden.shape[1]
    blocks = ff // SILU_BLOCK
    copies = [
        pltpu.make_async_copy(rest.at[:, 2 * ff : 2 * ff + key_width], outs, out_sem),
        pltpu.make_async_copy(tokens, held, token_sem),
    ]
    for k in range(blocks):
        for part in range(2):
            at = part * ff + k * SILU_BLOCK
            copies.append(
                pltpu.make_async_copy(
                    rest.at[:, at : at + SILU_BLOCK],
                    gates.at[k, :, part * SILU_BLOCK : (part + 1) * SILU_BLOCK],
                    gate_sems.at[k, part],
                )
            )
    copies.append(pltpu.make_async_copy(rest.at[:, 2 * ff + key_width :], downs, down_sem))
    for copy in copies:
        copy.start()
    step = 512
    nt = (((1,), (1,)), ((), ()))
    squares[...] = jnp.zeros_like(squares)
    copies[0].wait()
    copies[1].wait()

    def add_attended(k, carry):
        at = pl.ds(pl.multiple_of(k * step, step), step)
        product = lax.dot_general(
            attended[...], outs[at, :], nt, preferred_element_type=jnp.float32
        )
        total = (held[:, at].astype(jnp.float32) + product).astype(jnp.bfloat16)
        resid[:, at] = total
        total = total.astype(jnp.float32)
        total = total * total
        squares[...] += sum(total[:, j * 128 : (j + 1) * 128] for j in range(step // 128))
        return carry

    lax.fori_loop(0, depth // step, add_attended, 0)
    power = jnp.sum(squares[...], axis=1, keepdims=True) * (1.0 / depth)
    squares[...] = jnp.broadcast_to(lax.rsqrt(power + EPS), squares.shape)

    def scale(k, carry):
        at = pl.ds(pl.multiple_of(k * 128, 128), 128)
        normed[:, at] = (
            resid[:, at].astype(jnp.float32) * squares[...] * gain[:, at]
        ).astype(jnp.bfloat16)
        return carry

    lax.fori_loop(0, depth // 128, scale, 0)
    for k in range(blocks):
        copies[2 + 2 * k].wait()
        copies[3 + 2 * k].wait()
        both = jnp.dot(normed[...], gates[k], preferred_element_type=jnp.float32)
        gate = both[:, :SILU_BLOCK]
        hidden[:, k * SILU_BLOCK : (k + 1) * SILU_BLOCK] = (
            gate / (1.0 + jnp.exp(-gate)) * both[:, SILU_BLOCK:]
        ).astype(jnp.bfloat16)
    copies[-1].wait()

    def leave(k, slot):
        at = pl.ds(pl.multiple_of(k * step, step), step)
        return pltpu.make_async_copy(staged.at[slot], mixed.at[:, at], stage_sems.at[slot])

    def add_hidden(k, carry):
        slot = lax.rem(k, 2)
        at = pl.ds(pl.multiple_of(k * step, step), step)
        product = lax.dot_general(hidden[...], downs[at, :], nt, preferred_element_type=jnp.float32)

        @pl.when(k >= 2)
        def _():
            leave(k - 2, slot).wait()

        staged[slot] = (resid[:, at].astype(jnp.float32) + product).astype(jnp.bfloat16)
        leave(k, slot).start()
        return carry

    last = depth // step
    lax.fori_loop(0, last, add_hidden, 0)
    leave(last - 2, 0).wait()
    leave(last - 1, 1).wait()


def mlp(attended, gain, tokens, rest, ff):
    rows, depth = tokens.shape
    key_width = attended.shape[1]
    vmem = pl.BlockSpec(memory_space=pltpu.VMEM)
    hbm = pl.BlockSpec(memory_space=pl.ANY)
    blocks = ff // SILU_BLOCK
    bf16 = jnp.bfloat16
    return pl.pallas_call(
        mlp_kernel,
        out_shape=jax.ShapeDtypeStruct((rows, depth), bf16),
        in_specs=[vmem, vmem, hbm, hbm],
        out_specs=hbm,
        scratch_shapes=[
            pltpu.VMEM((rows, depth), bf16),
            pltpu.VMEM((blocks, depth, 2 * SILU_BLOCK), bf16),
            pltpu.VMEM((depth, key_width), bf16),
            pltpu.VMEM((depth, ff), bf16),
            pltpu.VMEM((rows, depth), bf16),
            pltpu.VMEM((rows, depth), bf16),
            pltpu.VMEM((rows, ff), bf16),
            pltpu.VMEM((rows, 128), jnp.float32),
            pltpu.VMEM((2, rows, 512), bf16),
            pltpu.SemaphoreType.DMA,
            pltpu.SemaphoreType.DMA,
            pltpu.SemaphoreType.DMA((blocks, 2)),
            pltpu.SemaphoreType.DMA,
            pltpu.SemaphoreType.DMA((2,)),
        ],
        compiler_params=pltpu.CompilerParams(vmem_limit_bytes=60 << 20),
        cost_estimate=pl.CostEstimate(
            flops=2 * rows * depth * (key_width + 3 * ff),
            bytes_accessed=2 * depth * (key_width + 3 * ff),
            transcendentals=rows * ff,
        ),
        name="mlp",
    )(attended, gain, tokens, rest)


def per_device(
    tokens, doc_ids, attn_gain, mlp_gain, w_query, w_key_value, w_out, w_gate, w_up, w_down
):
    rows = tokens.shape[0]
    rank = lax.axis_index(RANKS)
    ff = w_gate.shape[1]
    rest = jnp.concatenate([w_gate, w_up, w_out.T, w_down.T], axis=1)
    rest = lax.all_gather(rest, RANKS, axis=0, tiled=True)

    normed = rms_scale(tokens, attn_gain)
    query_width = w_query.shape[1]
    pair_width = w_key_value.shape[1]
    head = pair_width // 2
    heads = query_width // head
    pieces = gathered_pieces(jnp.concatenate([w_query, w_key_value], axis=1))
    position = rank * rows + jnp.arange(rows, dtype=jnp.int32)
    freqs = THETA ** (-2.0 * jnp.arange(head // 2, dtype=jnp.float32) / head)
    angle = position.astype(jnp.float32)[:, None] * freqs[None, :]
    cosine = jnp.cos(angle)
    sine = jnp.sin(angle)
    marks = doc_ids + 1
    mark_rows = jnp.pad(
        marks.astype(jnp.bfloat16).reshape(-1, pair_width),
        ((0, MARK_ROWS - rows // pair_width), (0, 0)),
    )
    coords = jnp.stack([lax.axis_index(name) for name in ("x", "y", "z", "core")]).astype(jnp.int32)
    query, sent = project(
        coords,
        normed,
        jnp.concatenate([cosine, cosine], axis=1),
        jnp.concatenate([-sine, sine], axis=1),
        mark_rows,
        pieces,
        w_query.shape[0],
        query_width,
        pair_width,
    )
    query = query.reshape(rows, heads, head)
    own_pairs = sent[:rows]
    pair_pieces = []
    mark_pieces = []
    for distance in range(SPAN, 0, -1):
        moved = shifted(sent, RANKS, distance)
        pair_pieces.append(moved[:rows])
        mark_pieces.append(
            moved[rows : rows + rows // pair_width].reshape(-1).astype(jnp.int32)
        )
    halo_pairs = jnp.concatenate(pair_pieces, axis=0)
    halo_marks = jnp.concatenate(mark_pieces, axis=0)
    mixed = attend_live(query, halo_pairs, halo_marks, own_pairs, marks, rows)
    attended = mixed.reshape(rows, query_width).astype(jnp.bfloat16)
    return mlp(attended, mlp_gain[None, :], tokens, rest, ff)


def solution(mesh):
    chips = Mesh(mesh.devices.reshape(RING, RING, 2, RING), RANKS)
    in_specs = (
        P(RANKS, None),
        P(RANKS),
        P(),
        P(),
        P(RANKS, None),
        P(RANKS, None),
        P(None, RANKS),
        P(RANKS, None),
        P(RANKS, None),
        P(None, RANKS),
    )
    out_specs = P(RANKS, None)
    return jax.shard_map(
        per_device, mesh=chips, in_specs=in_specs, out_specs=out_specs, check_vma=False
    )
```

```python
import functools
import math

import jax
import jax.numpy as jnp
from jax import lax
from jax.experimental import pallas as pl
from jax.experimental.pallas import tpu as pltpu
from jax.sharding import Mesh
from jax.sharding import PartitionSpec as P

SPAN = 4


EPS = 1e-05
THETA = 500000.0
NEGATIVE = -1e30
RANKS = ("y", "z", "core", "x")
RING = 4
DELTAS = (0, -1, 1, 2)
MARK_ROWS = 16
SILU_BLOCK = 256


def shifted(array, axis, by):
    length = lax.axis_size(axis)
    pairs = [(i, i + by) for i in range(length) if 0 <= i + by < length]
    return lax.ppermute(array, axis, pairs)


def turned(array, axis, by):
    return lax.ppermute(array, axis, [(i, (i + by) % RING) for i in range(RING)])


def swapped(array):
    return lax.ppermute(array, "core", [(0, 1), (1, 0)])


def rms_scale(values, gain):
    wide = values.astype(jnp.float32)
    power = jnp.mean(wide * wide, axis=-1, keepdims=True)
    return (wide * lax.rsqrt(power + EPS) * gain).astype(jnp.bfloat16)


def attend_kernel(head, query, marks, *refs):
    blocks = refs[:-4]
    attended, bias, scores, weights = refs[-4:]
    rows = query.shape[0]
    tile = 128
    per_row = blocks[0].shape[1] // tile
    for k, block in enumerate(blocks):
        for part in range(rows // tile):
            line = block[rows + part // per_row : rows + part // per_row + 1, :].astype(jnp.float32)
            line = line[:, (part % per_row) * tile : (part % per_row + 1) * tile]
            column = jnp.transpose(jnp.broadcast_to(line, (tile, tile)))
            for lane in range(rows // tile):
                same = column == marks[:, lane * tile : (lane + 1) * tile]
                if k == 0:
                    key = lax.broadcasted_iota(jnp.int32, (tile, tile), 0) + part * tile
                    place = lax.broadcasted_iota(jnp.int32, (tile, tile), 1) + lane * tile
                    same = same & (key <= place)
                bias[
                    k * rows + part * tile : k * rows + (part + 1) * tile,
                    lane * tile : (lane + 1) * tile,
                ] = jnp.where(same, 0.0, NEGATIVE)
    factor = 1.0 / math.sqrt(head)

    def one_head(h, carry):
        at = pl.ds(pl.multiple_of(h * head, head), head)
        peak = jnp.full((1, rows), NEGATIVE, jnp.float32)
        for k, block in enumerate(blocks):
            raw = lax.dot_general(
                block[:rows, :head],
                query[:, at],
                (((1,), (1,)), ((), ())),
                preferred_element_type=jnp.float32,
            )
            raw = raw * factor + bias[k * rows : (k + 1) * rows, :]
            scores[k * rows : (k + 1) * rows, :] = raw
            peak = jnp.maximum(peak, jnp.max(raw, axis=0, keepdims=True))
        totals = jnp.zeros((1, rows), jnp.float32)
        mixed = jnp.zeros((head, rows), jnp.float32)
        for k, block in enumerate(blocks):
            weight = jnp.exp(scores[k * rows : (k + 1) * rows, :] - peak)
            totals += jnp.sum(weight, axis=0, keepdims=True)
            weights[...] = weight.astype(jnp.bfloat16)
            mixed += lax.dot_general(
                block[:rows, head:],
                weights[...],
                (((0,), (0,)), ((), ())),
                preferred_element_type=jnp.float32,
            )
        attended[:, at] = jnp.transpose(mixed / totals).astype(jnp.bfloat16)
        return carry

    lax.fori_loop(0, query.shape[1] // head, one_head, 0)


def attend(query, marks, blocks):
    rows, width = query.shape
    head = blocks[0].shape[1] // 2
    keys = rows * len(blocks)
    vmem = pl.BlockSpec(memory_space=pltpu.VMEM)
    return pl.pallas_call(
        functools.partial(attend_kernel, head),
        out_shape=jax.ShapeDtypeStruct((rows, width), jnp.bfloat16),
        in_specs=[vmem] * (2 + len(blocks)),
        out_specs=vmem,
        scratch_shapes=[
            pltpu.VMEM((keys, rows), jnp.float32),
            pltpu.VMEM((keys, rows), jnp.float32),
            pltpu.VMEM((rows, rows), jnp.bfloat16),
        ],
        compiler_params=pltpu.CompilerParams(vmem_limit_bytes=32 << 20),
        cost_estimate=pl.CostEstimate(
            flops=4 * rows * keys * width,
            bytes_accessed=4 * rows * width + 4 * keys * head,
            transcendentals=keys * rows * (width // head),
        ),
        name="attend",
    )(query, marks, *blocks)


def gathered_near(block, axis):
    return jnp.concatenate([block] + [turned(block, axis, -d) for d in DELTAS[1:]], axis=0)


def gathered_pieces(shard):
    block = gathered_near(gathered_near(shard, "x"), "y")
    half = block.shape[0] // 2
    low = turned(block, "z", 1)
    high = turned(block, "z", -1)
    far_low = turned(low[:half], "z", 1)
    far_high = turned(high[half:], "z", -1)
    pieces = (block, low, high, far_low, far_high)
    return pieces + tuple(swapped(piece) for piece in pieces)


def load_pieces(coords, pieces, target, sem, unit):
    x, y, z, core = (coords[k] for k in range(4))
    count = len(pieces) // 2
    for swap in range(2):
        block, low, high, far_low, far_high = pieces[swap * count : (swap + 1) * count]
        owner = lax.rem(core + swap, 2)
        for pz in range(RING):
            from_z = lax.rem(z + DELTAS[pz] + RING, RING)
            for py in range(RING):
                from_y = lax.rem(y + DELTAS[py] + RING, RING)
                for px in range(RING):
                    from_x = lax.rem(x + DELTAS[px] + RING, RING)
                    rank = ((from_y * RING + from_z) * 2 + owner) * RING + from_x
                    place = py * RING + px
                    if pz < 3:
                        source = (block, low, high)[pz]
                    else:
                        source = far_low if place < 8 else far_high
                        place = place % 8
                    pltpu.make_async_copy(
                        source.at[pl.ds(place * unit, unit)],
                        target.at[pl.ds(pl.multiple_of(rank * unit, unit), unit)],
                        sem,
                    ).start()


def project_kernel(head, unit, *refs):
    coords, normed, cosine, sine, mark_rows = refs[:5]
    pieces = refs[5:15]
    query, pairs, weights, sem = refs[15:]
    load_pieces(coords, pieces, weights, sem, unit)
    rows = normed.shape[0]
    width = query.shape[1]
    pltpu.make_async_copy(weights, weights, sem).wait()

    def rotated(raw):
        return raw * cosine[...] + pltpu.roll(raw, head // 2, 1) * sine[...]

    pair_raw = jnp.dot(normed[...], weights[:, width:], preferred_element_type=jnp.float32)
    pairs[:rows, :head] = rotated(pair_raw[:, :head]).astype(jnp.bfloat16)
    pairs[:rows, head:] = pair_raw[:, head:].astype(jnp.bfloat16)
    pairs[rows:, :] = mark_rows[...]
    for begin in range(0, width, 2 * head):
        raw = jnp.dot(
            normed[...], weights[:, begin : begin + 2 * head], preferred_element_type=jnp.float32
        )
        for part in range(2):
            query[:, begin + part * head : begin + (part + 1) * head] = rotated(
                raw[:, part * head : (part + 1) * head]
            ).astype(jnp.bfloat16)


def project(coords, normed, cosine, sine, mark_rows, pieces, unit, query_width, pair_width):
    rows, depth = normed.shape
    vmem = pl.BlockSpec(memory_space=pltpu.VMEM)
    hbm = pl.BlockSpec(memory_space=pl.ANY)
    return pl.pallas_call(
        functools.partial(project_kernel, pair_width // 2, unit),
        out_shape=(
            jax.ShapeDtypeStruct((rows, query_width), jnp.bfloat16),
            jax.ShapeDtypeStruct((rows + MARK_ROWS, pair_width), jnp.bfloat16),
        ),
        in_specs=[pl.BlockSpec(memory_space=pltpu.SMEM)] + [vmem] * 4 + [hbm] * len(pieces),
        out_specs=(vmem, vmem),
        scratch_shapes=[
            pltpu.VMEM((depth, query_width + pair_width), jnp.bfloat16),
            pltpu.SemaphoreType.DMA,
        ],
        compiler_params=pltpu.CompilerParams(vmem_limit_bytes=40 << 20),
        cost_estimate=pl.CostEstimate(
            flops=2 * rows * depth * (query_width + pair_width),
            bytes_accessed=2 * depth * (query_width + pair_width),
            transcendentals=0,
        ),
        name="project",
    )(coords, normed, cosine, sine, mark_rows, *pieces)


def mlp_kernel(
    attended, gain, tokens, rest, mixed,
    held, gates, outs, downs, resid, normed, hidden, squares, staged,
    out_sems, gate_sems, down_sem, stage_sems,
):
    rows, depth = tokens.shape
    key_width = attended.shape[1]
    ff = hidden.shape[1]
    blocks = ff // SILU_BLOCK
    step = 512
    last = depth // step
    nt = (((1,), (1,)), ((), ()))

    def bring_out(k):
        at = pl.ds(pl.multiple_of(k * step, step), step)
        return (
            pltpu.make_async_copy(
                rest.at[at, 2 * ff : 2 * ff + key_width], outs.at[at], out_sems.at[k, 0]
            ),
            pltpu.make_async_copy(tokens.at[:, at], held.at[:, at], out_sems.at[k, 1]),
        )

    def bring_gate(k, part):
        at = part * ff + k * SILU_BLOCK
        return pltpu.make_async_copy(
            rest.at[:, at : at + SILU_BLOCK],
            gates.at[k, :, part * SILU_BLOCK : (part + 1) * SILU_BLOCK],
            gate_sems.at[k, part],
        )

    bring_down = pltpu.make_async_copy(rest.at[:, 2 * ff + key_width :], downs, down_sem)
    for k in range(last):
        for copy in bring_out(k):
            copy.start()
    squares[...] = jnp.zeros_like(squares)

    def add_attended(k, carry):
        at = pl.ds(pl.multiple_of(k * step, step), step)
        for copy in bring_out(k):
            copy.wait()
        product = lax.dot_general(
            attended[...], outs[at, :], nt, preferred_element_type=jnp.float32
        )
        total = (held[:, at].astype(jnp.float32) + product).astype(jnp.bfloat16)
        resid[:, at] = total
        total = total.astype(jnp.float32)
        total = total * total
        squares[...] += sum(total[:, j * 128 : (j + 1) * 128] for j in range(step // 128))
        return carry

    lax.fori_loop(0, 4, add_attended, 0)
    for k in range(blocks):
        bring_gate(k, 0).start()
        bring_gate(k, 1).start()
    lax.fori_loop(4, last, add_attended, 0)
    power = jnp.sum(squares[...], axis=1, keepdims=True) * (1.0 / depth)
    squares[...] = jnp.broadcast_to(lax.rsqrt(power + EPS), squares.shape)

    def scale(k, carry):
        at = pl.ds(pl.multiple_of(k * 128, 128), 128)
        normed[:, at] = (
            resid[:, at].astype(jnp.float32) * squares[...] * gain[:, at]
        ).astype(jnp.bfloat16)
        return carry

    lax.fori_loop(0, depth // 128, scale, 0)
    for k in range(blocks):
        bring_gate(k, 0).wait()
        bring_gate(k, 1).wait()
        if k == 0:
            bring_down.start()
        both = jnp.dot(normed[...], gates[k], preferred_element_type=jnp.float32)
        gate = both[:, :SILU_BLOCK]
        hidden[:, k * SILU_BLOCK : (k + 1) * SILU_BLOCK] = (
            gate / (1.0 + jnp.exp(-gate)) * both[:, SILU_BLOCK:]
        ).astype(jnp.bfloat16)
    bring_down.wait()

    def leave(k, slot):
        at = pl.ds(pl.multiple_of(k * step, step), step)
        return pltpu.make_async_copy(staged.at[slot], mixed.at[:, at], stage_sems.at[slot])

    def add_hidden(k, carry):
        slot = lax.rem(k, 2)
        at = pl.ds(pl.multiple_of(k * step, step), step)
        product = lax.dot_general(hidden[...], downs[at, :], nt, preferred_element_type=jnp.float32)

        @pl.when(k >= 2)
        def _():
            leave(k - 2, slot).wait()

        staged[slot] = (resid[:, at].astype(jnp.float32) + product).astype(jnp.bfloat16)
        leave(k, slot).start()
        return carry

    lax.fori_loop(0, last, add_hidden, 0)
    leave(last - 2, 0).wait()
    leave(last - 1, 1).wait()


def mlp(attended, gain, tokens, rest, ff):
    rows, depth = tokens.shape
    key_width = attended.shape[1]
    vmem = pl.BlockSpec(memory_space=pltpu.VMEM)
    hbm = pl.BlockSpec(memory_space=pl.ANY)
    blocks = ff // SILU_BLOCK
    bf16 = jnp.bfloat16
    return pl.pallas_call(
        mlp_kernel,
        out_shape=jax.ShapeDtypeStruct((rows, depth), bf16),
        in_specs=[vmem, vmem, hbm, hbm],
        out_specs=hbm,
        scratch_shapes=[
            pltpu.VMEM((rows, depth), bf16),
            pltpu.VMEM((blocks, depth, 2 * SILU_BLOCK), bf16),
            pltpu.VMEM((depth, key_width), bf16),
            pltpu.VMEM((depth, ff), bf16),
            pltpu.VMEM((rows, depth), bf16),
            pltpu.VMEM((rows, depth), bf16),
            pltpu.VMEM((rows, ff), bf16),
            pltpu.VMEM((rows, 128), jnp.float32),
            pltpu.VMEM((2, rows, 512), bf16),
            pltpu.SemaphoreType.DMA((depth // 512, 2)),
            pltpu.SemaphoreType.DMA((blocks, 2)),
            pltpu.SemaphoreType.DMA,
            pltpu.SemaphoreType.DMA((2,)),
        ],
        compiler_params=pltpu.CompilerParams(vmem_limit_bytes=60 << 20),
        cost_estimate=pl.CostEstimate(
            flops=2 * rows * depth * (key_width + 3 * ff),
            bytes_accessed=2 * depth * (key_width + 3 * ff),
            transcendentals=rows * ff,
        ),
        name="mlp",
    )(attended, gain, tokens, rest)


def per_device(
    tokens, doc_ids, attn_gain, mlp_gain, w_query, w_key_value, w_out, w_gate, w_up, w_down
):
    rows = tokens.shape[0]
    rank = lax.axis_index(RANKS)
    ff = w_gate.shape[1]
    rest = jnp.concatenate([w_gate, w_up, w_out.T, w_down.T], axis=1)
    rest = lax.all_gather(rest, RANKS, axis=0, tiled=True)

    normed = rms_scale(tokens, attn_gain)
    query_width = w_query.shape[1]
    pair_width = w_key_value.shape[1]
    head = pair_width // 2
    pieces = gathered_pieces(jnp.concatenate([w_query, w_key_value], axis=1))
    position = rank * rows + jnp.arange(rows, dtype=jnp.int32)
    freqs = THETA ** (-2.0 * jnp.arange(head // 2, dtype=jnp.float32) / head)
    angle = position.astype(jnp.float32)[:, None] * freqs[None, :]
    cosine = jnp.cos(angle)
    sine = jnp.sin(angle)
    marks = doc_ids + 1
    mark_rows = jnp.pad(
        marks.astype(jnp.bfloat16).reshape(-1, pair_width),
        ((0, MARK_ROWS - rows // pair_width), (0, 0)),
    )
    coords = jnp.stack([lax.axis_index(name) for name in ("x", "y", "z", "core")]).astype(jnp.int32)
    query, sent = project(
        coords,
        normed,
        jnp.concatenate([cosine, cosine], axis=1),
        jnp.concatenate([-sine, sine], axis=1),
        mark_rows,
        pieces,
        w_query.shape[0],
        query_width,
        pair_width,
    )
    halos = [shifted(sent, RANKS, distance) for distance in range(1, SPAN + 1)]
    attended = attend(query, marks.astype(jnp.float32)[None, :], [sent] + halos)
    return mlp(attended, mlp_gain[None, :], tokens, rest, ff)


def solution(mesh):
    chips = Mesh(mesh.devices.reshape(RING, RING, 2, RING), RANKS)
    in_specs = (
        P(RANKS, None),
        P(RANKS),
        P(),
        P(),
        P(RANKS, None),
        P(RANKS, None),
        P(None, RANKS),
        P(RANKS, None),
        P(RANKS, None),
        P(None, RANKS),
    )
    out_specs = P(RANKS, None)
    return jax.shard_map(
        per_device, mesh=chips, in_specs=in_specs, out_specs=out_specs, check_vma=False
    )
```

```python
import functools
import math

import jax
import jax.numpy as jnp
from jax import lax
from jax.experimental import pallas as pl
from jax.experimental.pallas import tpu as pltpu
from jax.sharding import Mesh
from jax.sharding import PartitionSpec as P

SPAN = 4


EPS = 1e-05
THETA = 500000.0
NEGATIVE = -1e30
RANKS = ("y", "z", "core", "x")
RING = 4
DELTAS = (0, -1, 1, 2)
MARK_ROWS = 16
SILU_BLOCK = 256
QUARTERS = 4


VMEM = pl.BlockSpec(memory_space=pltpu.VMEM)
SMEM = pl.BlockSpec(memory_space=pltpu.SMEM)
HBM = pl.BlockSpec(memory_space=pl.ANY)


def shifted(array, axis, by):
    length = lax.axis_size(axis)
    pairs = [(i, i + by) for i in range(length) if 0 <= i + by < length]
    return lax.ppermute(array, axis, pairs)


def turned(array, axis, by):
    return lax.ppermute(array, axis, [(i, (i + by) % RING) for i in range(RING)])


def rms_scale(values, gain):
    wide = values.astype(jnp.float32)
    power = jnp.mean(wide * wide, axis=-1, keepdims=True)
    return (wide * lax.rsqrt(power + EPS) * gain).astype(jnp.bfloat16)


def attend_kernel(head, query, marks, *refs):
    blocks = refs[:-4]
    attended, bias, scores, weights = refs[-4:]
    rows = query.shape[0]
    tile = 128
    per_row = blocks[0].shape[1] // tile
    for k, block in enumerate(blocks):
        for part in range(rows // tile):
            line = block[rows + part // per_row : rows + part // per_row + 1, :].astype(jnp.float32)
            line = line[:, (part % per_row) * tile : (part % per_row + 1) * tile]
            column = jnp.transpose(jnp.broadcast_to(line, (tile, tile)))
            for lane in range(rows // tile):
                same = column == marks[:, lane * tile : (lane + 1) * tile]
                if k == 0:
                    key = lax.broadcasted_iota(jnp.int32, (tile, tile), 0) + part * tile
                    place = lax.broadcasted_iota(jnp.int32, (tile, tile), 1) + lane * tile
                    same = same & (key <= place)
                bias[
                    k * rows + part * tile : k * rows + (part + 1) * tile,
                    lane * tile : (lane + 1) * tile,
                ] = jnp.where(same, 0.0, NEGATIVE)
    factor = 1.0 / math.sqrt(head)

    def one_head(h, carry):
        at = pl.ds(pl.multiple_of(h * head, head), head)
        peak = jnp.full((1, rows), NEGATIVE, jnp.float32)
        for k, block in enumerate(blocks):
            raw = lax.dot_general(
                block[:rows, :head],
                query[:, at],
                (((1,), (1,)), ((), ())),
                preferred_element_type=jnp.float32,
            )
            raw = raw * factor + bias[k * rows : (k + 1) * rows, :]
            scores[k * rows : (k + 1) * rows, :] = raw
            peak = jnp.maximum(peak, jnp.max(raw, axis=0, keepdims=True))
        totals = jnp.zeros((1, rows), jnp.float32)
        mixed = jnp.zeros((head, rows), jnp.float32)
        for k, block in enumerate(blocks):
            weight = jnp.exp(scores[k * rows : (k + 1) * rows, :] - peak)
            totals += jnp.sum(weight, axis=0, keepdims=True)
            weights[...] = weight.astype(jnp.bfloat16)
            mixed += lax.dot_general(
                block[:rows, head:],
                weights[...],
                (((0,), (0,)), ((), ())),
                preferred_element_type=jnp.float32,
            )
        attended[:, at] = jnp.transpose(mixed / totals).astype(jnp.bfloat16)
        return carry

    lax.fori_loop(0, query.shape[1] // head, one_head, 0)


def attend(query, marks, blocks):
    rows, width = query.shape
    head = blocks[0].shape[1] // 2
    keys = rows * len(blocks)
    vmem = pl.BlockSpec(memory_space=pltpu.VMEM)
    return pl.pallas_call(
        functools.partial(attend_kernel, head),
        out_shape=jax.ShapeDtypeStruct((rows, width), jnp.bfloat16),
        in_specs=[vmem] * (2 + len(blocks)),
        out_specs=vmem,
        scratch_shapes=[
            pltpu.VMEM((keys, rows), jnp.float32),
            pltpu.VMEM((keys, rows), jnp.float32),
            pltpu.VMEM((rows, rows), jnp.bfloat16),
        ],
        compiler_params=pltpu.CompilerParams(vmem_limit_bytes=32 << 20),
        cost_estimate=pl.CostEstimate(
            flops=4 * rows * keys * width,
            bytes_accessed=4 * rows * width + 4 * keys * head,
            transcendentals=keys * rows * (width // head),
        ),
        name="attend",
    )(query, marks, *blocks)


def place_kernel(splits, me, *refs):
    pieces, outs = refs[:RING], refs[RING:]
    rows = pieces[0].shape[0]
    for k, piece in enumerate(pieces):
        at = pl.ds(pl.multiple_of(lax.rem(me[0] + k, RING) * rows, rows), rows)
        for out, begin, end in zip(outs, splits, splits[1:]):
            out[at, :] = piece[:, begin:end]


def gathered(block, axis, splits):
    pieces = [block] + [turned(block, axis, -k) for k in range(1, RING)]
    rows = block.shape[0]
    return pl.pallas_call(
        functools.partial(place_kernel, splits),
        out_shape=tuple(
            jax.ShapeDtypeStruct((RING * rows, end - begin), block.dtype)
            for begin, end in zip(splits, splits[1:])
        ),
        in_specs=[SMEM] + [VMEM] * RING,
        out_specs=tuple(VMEM for _ in splits[1:]),
        compiler_params=pltpu.CompilerParams(vmem_limit_bytes=8 << 20),
        cost_estimate=pl.CostEstimate(
            flops=RING * block.size, bytes_accessed=4 * RING * block.size, transcendentals=0
        ),
        name="place",
    )(lax.axis_index(axis).astype(jnp.int32)[None], *pieces)


def first_step(block, axis):
    return block, turned(block, axis, 1), turned(block, axis, -1)


def second_step(block, low, high, axis):
    half = block.shape[0] // 2
    far_low = turned(low[:half], axis, 1)
    far_high = turned(high[half:], axis, -1)
    pieces = (block, low, high, far_low, far_high)
    swap = [(0, 1), (1, 0)]
    return pieces + tuple(lax.ppermute(piece, "core", swap) for piece in pieces)


def load_pieces(coords, pieces, target, sem, unit):
    count = len(pieces) // 2

    line = RING * unit
    for swap in range(2):
        block, low, high, far_low, far_high = pieces[swap * count : (swap + 1) * count]
        owner = lax.rem(coords[3] + swap, 2)
        for outer in range(RING):
            from_z = lax.rem(coords[2] + DELTAS[outer] + RING, RING)
            for inner in range(RING):
                piece = (block, low, high, (far_low, far_high)[inner // 2])[outer]
                begin = (inner % 2 if outer == 3 else inner) * line
                place = ((inner * RING + from_z) * 2 + owner) * line
                pltpu.make_async_copy(
                    piece.at[pl.ds(begin, line)],
                    target.at[pl.ds(pl.multiple_of(place, line), line)],
                    sem,
                ).start()


def rotated(raw, cosine, sine):
    return raw * cosine[...] + pltpu.roll(raw, raw.shape[1] // 2, 1) * sine[...]


def project_pairs_kernel(unit, coords, normed, cosine, sine, mark_rows, *refs):
    pieces = refs[:-3]
    pairs, weights, sem = refs[-3:]
    load_pieces(coords, pieces, weights, sem, unit)
    rows = normed.shape[0]
    head = pairs.shape[1] // 2
    pairs[rows:, :] = mark_rows[...]
    pltpu.make_async_copy(weights, weights, sem).wait()
    raw = jnp.dot(normed[...], weights[...], preferred_element_type=jnp.float32)
    pairs[:rows, :head] = rotated(raw[:, :head], cosine, sine).astype(jnp.bfloat16)
    pairs[:rows, head:] = raw[:, head:].astype(jnp.bfloat16)


def project_query_kernel(unit, coords, normed, cosine, sine, *refs):
    pieces = refs[:-3]
    query, weights, sem = refs[-3:]
    head = cosine.shape[1]
    load_pieces(coords, pieces, weights, sem, unit)
    pltpu.make_async_copy(weights, weights, sem).wait()
    raw = jnp.dot(normed[...], weights[...], preferred_element_type=jnp.float32)
    for begin in range(0, query.shape[1], head):
        query[:, begin : begin + head] = rotated(
            raw[:, begin : begin + head], cosine, sine
        ).astype(jnp.bfloat16)


def project(kernel, coords, held, pieces, unit, out_rows):
    rows, depth = held[0].shape
    width = pieces[0].shape[1]
    return pl.pallas_call(
        functools.partial(kernel, unit),
        out_shape=jax.ShapeDtypeStruct((out_rows, width), jnp.bfloat16),
        in_specs=[SMEM] + [VMEM] * len(held) + [HBM] * len(pieces),
        out_specs=VMEM,
        scratch_shapes=[
            pltpu.VMEM((depth, width), jnp.bfloat16),
            pltpu.SemaphoreType.DMA,
        ],
        compiler_params=pltpu.CompilerParams(vmem_limit_bytes=24 << 20),
        cost_estimate=pl.CostEstimate(
            flops=2 * rows * depth * width, bytes_accessed=2 * depth * width, transcendentals=0
        ),
    )(coords, *held, *pieces)


def out_kernel(unit, coords, attended, gain, tokens, *refs):
    pieces = refs[:10]
    resid_out, normed_out, held, outs, resid, normed, squares, token_sems, out_sem, leave_sems = refs[10:]
    _, depth = tokens.shape
    step = 512
    last = depth // step
    nt = (((1,), (1,)), ((), ()))
    load_pieces(coords, pieces, outs, out_sem, unit)

    def part(k):
        return pl.ds(pl.multiple_of(k * step, step), step)

    def bring(k):
        return pltpu.make_async_copy(tokens.at[:, part(k)], held.at[:, part(k)], token_sems.at[k])

    def leave(k, which):
        source, target = ((resid, resid_out), (normed, normed_out))[which]
        return pltpu.make_async_copy(
            source.at[:, part(k)], target.at[:, part(k)], leave_sems.at[k, which]
        )

    for k in range(last):
        bring(k).start()
    squares[...] = jnp.zeros_like(squares)
    pltpu.make_async_copy(outs, outs, out_sem).wait()

    def add_attended(k, carry):
        bring(k).wait()
        product = lax.dot_general(
            attended[...], outs[part(k), :], nt, preferred_element_type=jnp.float32
        )
        total = (held[:, part(k)].astype(jnp.float32) + product).astype(jnp.bfloat16)
        resid[:, part(k)] = total
        total = total.astype(jnp.float32)
        total = total * total
        squares[...] += sum(total[:, j * 128 : (j + 1) * 128] for j in range(step // 128))
        return carry

    lax.fori_loop(0, last, add_attended, 0)
    power = jnp.sum(squares[...], axis=1, keepdims=True) * (1.0 / depth)
    squares[...] = jnp.broadcast_to(lax.rsqrt(power + EPS), squares.shape)

    def scale(k, carry):
        leave(k, 0).start()
        for j in range(step // 128):
            at = pl.ds(pl.multiple_of(k * step + j * 128, 128), 128)
            normed[:, at] = (
                resid[:, at].astype(jnp.float32) * squares[...] * gain[:, at]
            ).astype(jnp.bfloat16)
        leave(k, 1).start()
        return carry

    lax.fori_loop(0, last, scale, 0)
    for k in range(last):
        leave(k, 0).wait()
        leave(k, 1).wait()


def add_out(coords, attended, gain, tokens, pieces, unit):
    rows, depth = tokens.shape
    key_width = attended.shape[1]
    whole = jax.ShapeDtypeStruct((rows, depth), jnp.bfloat16)
    held = pltpu.VMEM((rows, depth), jnp.bfloat16)
    return pl.pallas_call(
        functools.partial(out_kernel, unit),
        out_shape=(whole, whole),
        in_specs=[SMEM, VMEM, VMEM, HBM] + [HBM] * len(pieces),
        out_specs=(HBM, HBM),
        scratch_shapes=[
            held,
            pltpu.VMEM((depth, key_width), jnp.bfloat16),
            held,
            held,
            pltpu.VMEM((rows, 128), jnp.float32),
            pltpu.SemaphoreType.DMA((depth // 512,)),
            pltpu.SemaphoreType.DMA,
            pltpu.SemaphoreType.DMA((depth // 512, 2)),
        ],
        compiler_params=pltpu.CompilerParams(vmem_limit_bytes=56 << 20),
        cost_estimate=pl.CostEstimate(
            flops=2 * rows * depth * key_width,
            bytes_accessed=2 * depth * (key_width + 3 * rows),
            transcendentals=0,
        ),
        name="add_out",
    )(coords, attended, gain, tokens, *pieces)


def mlp_kernel(
    resid_hbm, normed_hbm, rest, mixed,
    resid, normed, gates, downs, hidden, staged,
    first_sems, gate_sems, down_sems, stage_sems,
):
    _, depth = resid.shape
    ff = hidden.shape[1]
    blocks = ff // SILU_BLOCK
    step = 512
    last = depth // step
    nt = (((1,), (1,)), ((), ()))

    def bring_gate(k, part):
        at = part * ff + k * SILU_BLOCK
        return pltpu.make_async_copy(
            rest.at[:, at : at + SILU_BLOCK],
            gates.at[k, :, part * SILU_BLOCK : (part + 1) * SILU_BLOCK],
            gate_sems.at[k, part],
        )

    def bring_down(k):
        at = pl.ds(pl.multiple_of(k * step, step), step)
        return (
            pltpu.make_async_copy(resid_hbm.at[:, at], resid.at[:, at], down_sems.at[k, 0]),
            pltpu.make_async_copy(
                rest.at[at, 2 * ff : 3 * ff], downs.at[at], down_sems.at[k, 1]
            ),
        )

    quarter = depth // QUARTERS

    def bring_first(q):
        at = slice(q * quarter, (q + 1) * quarter)
        return (
            pltpu.make_async_copy(normed_hbm.at[:, at], normed.at[:, at], first_sems.at[q, 0]),
            pltpu.make_async_copy(
                rest.at[at, :SILU_BLOCK], gates.at[0, at, :SILU_BLOCK], first_sems.at[q, 1]
            ),
            pltpu.make_async_copy(
                rest.at[at, ff : ff + SILU_BLOCK],
                gates.at[0, at, SILU_BLOCK:],
                first_sems.at[q, 2],
            ),
        )

    def start_down(k, carry):
        for copy in bring_down(k):
            copy.start()
        return carry

    def start_gate(k):
        if k < blocks:
            bring_gate(k, 0).start()
            bring_gate(k, 1).start()

    for q in range(QUARTERS):
        for copy in bring_first(q):
            copy.start()
    for k in range(blocks):
        if k == 0:
            both = 0.0
            for q in range(QUARTERS):
                for copy in bring_first(q):
                    copy.wait()
                if q == QUARTERS // 2:
                    start_gate(1)
                if q == QUARTERS - 1:
                    start_gate(2)
                at = slice(q * quarter, (q + 1) * quarter)
                both += jnp.dot(normed[:, at], gates[0, at], preferred_element_type=jnp.float32)
        else:
            bring_gate(k, 0).wait()
            bring_gate(k, 1).wait()
            start_gate(k + 2)
            if k == blocks - 2:
                lax.fori_loop(0, last // 2, start_down, 0)
            if k == blocks - 1:
                lax.fori_loop(last // 2, last, start_down, 0)
            both = jnp.dot(normed[...], gates[k], preferred_element_type=jnp.float32)
        gate = both[:, :SILU_BLOCK]
        hidden[:, k * SILU_BLOCK : (k + 1) * SILU_BLOCK] = (
            gate / (1.0 + jnp.exp(-gate)) * both[:, SILU_BLOCK:]
        ).astype(jnp.bfloat16)

    def leave(k, slot):
        at = pl.ds(pl.multiple_of(k * step, step), step)
        return pltpu.make_async_copy(staged.at[slot], mixed.at[:, at], stage_sems.at[slot])

    def add_hidden(k, carry):
        slot = lax.rem(k, 2)
        at = pl.ds(pl.multiple_of(k * step, step), step)
        for copy in bring_down(k):
            copy.wait()
        product = lax.dot_general(hidden[...], downs[at, :], nt, preferred_element_type=jnp.float32)

        @pl.when(k >= 2)
        def _():
            leave(k - 2, slot).wait()

        staged[slot] = (resid[:, at].astype(jnp.float32) + product).astype(jnp.bfloat16)
        leave(k, slot).start()
        return carry

    lax.fori_loop(0, last, add_hidden, 0)
    leave(last - 2, 0).wait()
    leave(last - 1, 1).wait()


def mlp(resid, normed, rest, ff):
    rows, depth = resid.shape
    blocks = ff // SILU_BLOCK
    bf16 = jnp.bfloat16
    return pl.pallas_call(
        mlp_kernel,
        out_shape=jax.ShapeDtypeStruct((rows, depth), bf16),
        in_specs=[HBM, HBM, HBM],
        out_specs=HBM,
        scratch_shapes=[
            pltpu.VMEM((rows, depth), bf16),
            pltpu.VMEM((rows, depth), bf16),
            pltpu.VMEM((blocks, depth, 2 * SILU_BLOCK), bf16),
            pltpu.VMEM((depth, ff), bf16),
            pltpu.VMEM((rows, ff), bf16),
            pltpu.VMEM((2, rows, 512), bf16),
            pltpu.SemaphoreType.DMA((QUARTERS, 3)),
            pltpu.SemaphoreType.DMA((blocks, 2)),
            pltpu.SemaphoreType.DMA((depth // 512, 2)),
            pltpu.SemaphoreType.DMA((2,)),
        ],
        compiler_params=pltpu.CompilerParams(vmem_limit_bytes=60 << 20),
        cost_estimate=pl.CostEstimate(
            flops=6 * rows * depth * ff,
            bytes_accessed=6 * depth * ff,
            transcendentals=rows * ff,
        ),
        name="mlp",
    )(resid, normed, rest)


def per_device(
    tokens, doc_ids, attn_gain, mlp_gain, w_query, w_key_value, w_out, w_gate, w_up, w_down
):
    rows = tokens.shape[0]
    rank = lax.axis_index(RANKS)
    ff = w_gate.shape[1]
    unit = w_gate.shape[0]
    rest = lax.all_gather(
        jnp.concatenate([w_gate, w_up, w_down.T], axis=1), RANKS, axis=0, tiled=True
    )

    query_width = w_query.shape[1]
    pair_width = w_key_value.shape[1]
    head = pair_width // 2
    normed = rms_scale(tokens, attn_gain)
    position = rank * rows + jnp.arange(rows, dtype=jnp.int32)
    freqs = THETA ** (-2.0 * jnp.arange(head // 2, dtype=jnp.float32) / head)
    angle = position.astype(jnp.float32)[:, None] * freqs[None, :]
    cosine = jnp.cos(angle)
    sine = jnp.sin(angle)
    cosine, sine = (
        jnp.concatenate([cosine, cosine], axis=1),
        jnp.concatenate([-sine, sine], axis=1),
    )
    marks = doc_ids + 1
    mark_rows = jnp.pad(
        marks.astype(jnp.bfloat16).reshape(-1, pair_width),
        ((0, MARK_ROWS - rows // pair_width), (0, 0)),
    )
    coords = jnp.stack([lax.axis_index(name) for name in ("x", "y", "z", "core")]).astype(jnp.int32)

    near = jnp.concatenate([w_query, w_key_value, w_out.T], axis=1)
    both = query_width + pair_width
    near, later = gathered(near, "x", (0, both, both + w_out.shape[0]))
    queries, pairs = gathered(near, "y", (0, query_width, both))
    pair_first = first_step(pairs, "z")
    pair_first, cosine, sine, mark_rows, coords = lax.optimization_barrier(
        (pair_first, cosine, sine, mark_rows, coords)
    )
    pair_pieces = second_step(*pair_first, "z")
    query_pieces = second_step(*first_step(queries, "z"), "z")
    (later,) = gathered(later, "y", (0, w_out.shape[0]))
    out_pieces = second_step(*first_step(later, "z"), "z")
    sent = project(
        project_pairs_kernel,
        coords,
        [normed, cosine, sine, mark_rows],
        pair_pieces,
        unit,
        rows + MARK_ROWS,
    )
    halos = [shifted(sent, RANKS, by) for by in range(1, SPAN + 1)]
    query = project(project_query_kernel, coords, [normed, cosine, sine], query_pieces, unit, rows)
    attended = attend(query, marks.astype(jnp.float32)[None, :], [sent] + halos)
    resid, normed_mlp = add_out(coords, attended, mlp_gain[None, :], tokens, out_pieces, unit)
    return mlp(resid, normed_mlp, rest, ff)


def solution(mesh):
    chips = Mesh(mesh.devices.reshape(RING, RING, 2, RING), RANKS)
    in_specs = (
        P(RANKS, None),
        P(RANKS),
        P(),
        P(),
        P(RANKS, None),
        P(RANKS, None),
        P(None, RANKS),
        P(RANKS, None),
        P(RANKS, None),
        P(None, RANKS),
    )
    out_specs = P(RANKS, None)
    return jax.shard_map(
        per_device, mesh=chips, in_specs=in_specs, out_specs=out_specs, check_vma=False
    )
```

```python
import functools
import math

import jax
import jax.numpy as jnp
from jax import lax
from jax.experimental import pallas as pl
from jax.experimental.pallas import tpu as pltpu
from jax.sharding import Mesh
from jax.sharding import PartitionSpec as P

SPAN = 4


EPS = 1e-05
THETA = 500000.0
NEGATIVE = -1e30
RANKS = ("y", "z", "core", "x")
RING = 4
DELTAS = (0, -1, 1, 2)
MARK_ROWS = 16
SILU_BLOCK = 256
QUARTERS = 4


VMEM = pl.BlockSpec(memory_space=pltpu.VMEM)
SMEM = pl.BlockSpec(memory_space=pltpu.SMEM)
HBM = pl.BlockSpec(memory_space=pl.ANY)


def shifted(array, axis, by):
    length = lax.axis_size(axis)
    pairs = [(i, i + by) for i in range(length) if 0 <= i + by < length]
    return lax.ppermute(array, axis, pairs)


def turned(array, axis, by):
    return lax.ppermute(array, axis, [(i, (i + by) % RING) for i in range(RING)])


def rms_scale(values, gain):
    wide = values.astype(jnp.float32)
    power = jnp.mean(wide * wide, axis=-1, keepdims=True)
    return (wide * lax.rsqrt(power + EPS) * gain).astype(jnp.bfloat16)


def attend_kernel(head, query, marks, *refs):
    blocks = refs[:-4]
    attended, bias, scores, weights = refs[-4:]
    rows = query.shape[0]
    tile = 128
    per_row = blocks[0].shape[1] // tile
    for k, block in enumerate(blocks):
        for part in range(rows // tile):
            line = block[rows + part // per_row : rows + part // per_row + 1, :].astype(jnp.float32)
            line = line[:, (part % per_row) * tile : (part % per_row + 1) * tile]
            column = jnp.transpose(jnp.broadcast_to(line, (tile, tile)))
            for lane in range(rows // tile):
                same = column == marks[:, lane * tile : (lane + 1) * tile]
                if k == 0:
                    key = lax.broadcasted_iota(jnp.int32, (tile, tile), 0) + part * tile
                    place = lax.broadcasted_iota(jnp.int32, (tile, tile), 1) + lane * tile
                    same = same & (key <= place)
                bias[
                    k * rows + part * tile : k * rows + (part + 1) * tile,
                    lane * tile : (lane + 1) * tile,
                ] = jnp.where(same, 0.0, NEGATIVE)
    factor = 1.0 / math.sqrt(head)

    def one_head(h, carry):
        at = pl.ds(pl.multiple_of(h * head, head), head)
        peak = jnp.full((1, rows), NEGATIVE, jnp.float32)
        for k, block in enumerate(blocks):
            raw = lax.dot_general(
                block[:rows, :head],
                query[:, at],
                (((1,), (1,)), ((), ())),
                preferred_element_type=jnp.float32,
            )
            raw = raw * factor + bias[k * rows : (k + 1) * rows, :]
            scores[k * rows : (k + 1) * rows, :] = raw
            peak = jnp.maximum(peak, jnp.max(raw, axis=0, keepdims=True))
        totals = jnp.zeros((1, rows), jnp.float32)
        mixed = jnp.zeros((head, rows), jnp.float32)
        for k, block in enumerate(blocks):
            weight = jnp.exp(scores[k * rows : (k + 1) * rows, :] - peak)
            totals += jnp.sum(weight, axis=0, keepdims=True)
            weights[...] = weight.astype(jnp.bfloat16)
            mixed += lax.dot_general(
                block[:rows, head:],
                weights[...],
                (((0,), (0,)), ((), ())),
                preferred_element_type=jnp.float32,
            )
        attended[:, at] = jnp.transpose(mixed / totals).astype(jnp.bfloat16)
        return carry

    lax.fori_loop(0, query.shape[1] // head, one_head, 0)


def attend(query, marks, blocks):
    rows, width = query.shape
    head = blocks[0].shape[1] // 2
    keys = rows * len(blocks)
    vmem = pl.BlockSpec(memory_space=pltpu.VMEM)
    return pl.pallas_call(
        functools.partial(attend_kernel, head),
        out_shape=jax.ShapeDtypeStruct((rows, width), jnp.bfloat16),
        in_specs=[vmem] * (2 + len(blocks)),
        out_specs=vmem,
        scratch_shapes=[
            pltpu.VMEM((keys, rows), jnp.float32),
            pltpu.VMEM((keys, rows), jnp.float32),
            pltpu.VMEM((rows, rows), jnp.bfloat16),
        ],
        compiler_params=pltpu.CompilerParams(vmem_limit_bytes=32 << 20),
        cost_estimate=pl.CostEstimate(
            flops=4 * rows * keys * width,
            bytes_accessed=4 * rows * width + 4 * keys * head,
            transcendentals=keys * rows * (width // head),
        ),
        name="attend",
    )(query, marks, *blocks)


def place_kernel(splits, me, *refs):
    pieces, outs = refs[:RING], refs[RING:]
    rows = pieces[0].shape[0]
    for k, piece in enumerate(pieces):
        at = pl.ds(pl.multiple_of(lax.rem(me[0] + k, RING) * rows, rows), rows)
        for out, begin, end in zip(outs, splits, splits[1:]):
            out[at, :] = piece[:, begin:end]


def gathered(block, axis, splits):
    pieces = [block] + [turned(block, axis, -k) for k in range(1, RING)]
    rows = block.shape[0]
    return pl.pallas_call(
        functools.partial(place_kernel, splits),
        out_shape=tuple(
            jax.ShapeDtypeStruct((RING * rows, end - begin), block.dtype)
            for begin, end in zip(splits, splits[1:])
        ),
        in_specs=[SMEM] + [VMEM] * RING,
        out_specs=tuple(VMEM for _ in splits[1:]),
        compiler_params=pltpu.CompilerParams(vmem_limit_bytes=8 << 20),
        cost_estimate=pl.CostEstimate(
            flops=RING * block.size, bytes_accessed=4 * RING * block.size, transcendentals=0
        ),
        name="place",
    )(lax.axis_index(axis).astype(jnp.int32)[None], *pieces)


def first_step(block, axis):
    return block, turned(block, axis, 1), turned(block, axis, -1)


def second_step(block, low, high, axis):
    half = block.shape[0] // 2
    far_low = turned(low[:half], axis, 1)
    far_high = turned(high[half:], axis, -1)
    pieces = (block, low, high, far_low, far_high)
    swap = [(0, 1), (1, 0)]
    return pieces + tuple(lax.ppermute(piece, "core", swap) for piece in pieces)


def load_pieces(coords, pieces, order, target, sem, unit):
    count = len(pieces) // 2
    whole = order[0] == "x"
    line = RING * unit if whole else unit
    last = "xyz".index(order[2])

    def bring_line(second, first, begin):
        for swap in range(2):
            block, low, high, far_low, far_high = pieces[swap * count : (swap + 1) * count]
            owner = lax.rem(coords[3] + swap, 2)
            for outer in range(RING):
                came = {order[0]: first, order[1]: second}
                came[order[2]] = lax.rem(coords[last] + DELTAS[outer] + RING, RING)
                rank = ((came["y"] * RING + came["z"]) * 2 + owner) * RING + came["x"]
                piece = (block, low, high, (far_low, far_high)[begin])[outer]
                row = second * RING * unit + (0 if whole else first * unit)
                if outer == 3:
                    row = row - begin * 2 * RING * unit
                pltpu.make_async_copy(
                    piece.at[pl.ds(pl.multiple_of(row, unit), line)],
                    target.at[pl.ds(pl.multiple_of(rank * unit, unit), line)],
                    sem,
                ).start()

    for begin in range(2):
        if whole:
            for second in range(2 * begin, 2 * begin + 2):
                bring_line(second, 0, begin)
        else:

            def step(k, carry):
                bring_line(2 * begin + k // RING, lax.rem(k, RING), begin)
                return carry

            lax.fori_loop(0, 2 * RING, step, 0)


def rotated(raw, cosine, sine):
    return raw * cosine[...] + pltpu.roll(raw, raw.shape[1] // 2, 1) * sine[...]


def project_pairs_kernel(unit, coords, normed, cosine, sine, mark_rows, *refs):
    pieces = refs[:-3]
    pairs, weights, sem = refs[-3:]
    load_pieces(coords, pieces, "xyz", weights, sem, unit)
    rows = normed.shape[0]
    head = pairs.shape[1] // 2
    pairs[rows:, :] = mark_rows[...]
    pltpu.make_async_copy(weights, weights, sem).wait()
    raw = jnp.dot(normed[...], weights[...], preferred_element_type=jnp.float32)
    pairs[:rows, :head] = rotated(raw[:, :head], cosine, sine).astype(jnp.bfloat16)
    pairs[:rows, head:] = raw[:, head:].astype(jnp.bfloat16)


def project_query_kernel(unit, coords, normed, cosine, sine, *refs):
    pieces = refs[:-3]
    query, weights, sem = refs[-3:]
    head = cosine.shape[1]
    load_pieces(coords, pieces, "xzy", weights, sem, unit)
    pltpu.make_async_copy(weights, weights, sem).wait()
    raw = jnp.dot(normed[...], weights[...], preferred_element_type=jnp.float32)
    for begin in range(0, query.shape[1], head):
        query[:, begin : begin + head] = rotated(
            raw[:, begin : begin + head], cosine, sine
        ).astype(jnp.bfloat16)


def project(kernel, coords, held, pieces, unit, out_rows):
    rows, depth = held[0].shape
    width = pieces[0].shape[1]
    return pl.pallas_call(
        functools.partial(kernel, unit),
        out_shape=jax.ShapeDtypeStruct((out_rows, width), jnp.bfloat16),
        in_specs=[SMEM] + [VMEM] * len(held) + [HBM] * len(pieces),
        out_specs=VMEM,
        scratch_shapes=[
            pltpu.VMEM((depth, width), jnp.bfloat16),
            pltpu.SemaphoreType.DMA,
        ],
        compiler_params=pltpu.CompilerParams(vmem_limit_bytes=24 << 20),
        cost_estimate=pl.CostEstimate(
            flops=2 * rows * depth * width, bytes_accessed=2 * depth * width, transcendentals=0
        ),
    )(coords, *held, *pieces)


def out_kernel(unit, coords, attended, gain, tokens, *refs):
    pieces = refs[:10]
    resid_out, normed_out, held, outs, resid, normed, squares, token_sems, out_sem, leave_sems = refs[10:]
    _, depth = tokens.shape
    step = 512
    last = depth // step
    nt = (((1,), (1,)), ((), ()))
    load_pieces(coords, pieces, "yzx", outs, out_sem, unit)

    def part(k):
        return pl.ds(pl.multiple_of(k * step, step), step)

    def bring(k):
        return pltpu.make_async_copy(tokens.at[:, part(k)], held.at[:, part(k)], token_sems.at[k])

    def leave(k, which):
        source, target = ((resid, resid_out), (normed, normed_out))[which]
        return pltpu.make_async_copy(
            source.at[:, part(k)], target.at[:, part(k)], leave_sems.at[k, which]
        )

    for k in range(last):
        bring(k).start()
    squares[...] = jnp.zeros_like(squares)
    pltpu.make_async_copy(outs, outs, out_sem).wait()

    def add_attended(k, carry):
        bring(k).wait()
        product = lax.dot_general(
            attended[...], outs[part(k), :], nt, preferred_element_type=jnp.float32
        )
        total = (held[:, part(k)].astype(jnp.float32) + product).astype(jnp.bfloat16)
        resid[:, part(k)] = total
        total = total.astype(jnp.float32)
        total = total * total
        squares[...] += sum(total[:, j * 128 : (j + 1) * 128] for j in range(step // 128))
        return carry

    lax.fori_loop(0, last, add_attended, 0)
    power = jnp.sum(squares[...], axis=1, keepdims=True) * (1.0 / depth)
    squares[...] = jnp.broadcast_to(lax.rsqrt(power + EPS), squares.shape)

    def scale(k, carry):
        leave(k, 0).start()
        for j in range(step // 128):
            at = pl.ds(pl.multiple_of(k * step + j * 128, 128), 128)
            normed[:, at] = (
                resid[:, at].astype(jnp.float32) * squares[...] * gain[:, at]
            ).astype(jnp.bfloat16)
        leave(k, 1).start()
        return carry

    lax.fori_loop(0, last, scale, 0)
    for k in range(last):
        leave(k, 0).wait()
        leave(k, 1).wait()


def add_out(coords, attended, gain, tokens, pieces, unit):
    rows, depth = tokens.shape
    key_width = attended.shape[1]
    whole = jax.ShapeDtypeStruct((rows, depth), jnp.bfloat16)
    held = pltpu.VMEM((rows, depth), jnp.bfloat16)
    return pl.pallas_call(
        functools.partial(out_kernel, unit),
        out_shape=(whole, whole),
        in_specs=[SMEM, VMEM, VMEM, HBM] + [HBM] * len(pieces),
        out_specs=(HBM, HBM),
        scratch_shapes=[
            held,
            pltpu.VMEM((depth, key_width), jnp.bfloat16),
            held,
            held,
            pltpu.VMEM((rows, 128), jnp.float32),
            pltpu.SemaphoreType.DMA((depth // 512,)),
            pltpu.SemaphoreType.DMA,
            pltpu.SemaphoreType.DMA((depth // 512, 2)),
        ],
        compiler_params=pltpu.CompilerParams(vmem_limit_bytes=56 << 20),
        cost_estimate=pl.CostEstimate(
            flops=2 * rows * depth * key_width,
            bytes_accessed=2 * depth * (key_width + 3 * rows),
            transcendentals=0,
        ),
        name="add_out",
    )(coords, attended, gain, tokens, *pieces)


def mlp_kernel(
    resid_hbm, normed_hbm, rest, mixed,
    resid, normed, gates, downs, hidden, staged,
    first_sems, gate_sems, down_sems, stage_sems,
):
    _, depth = resid.shape
    ff = hidden.shape[1]
    blocks = ff // SILU_BLOCK
    step = 512
    last = depth // step
    nt = (((1,), (1,)), ((), ()))

    def bring_gate(k, part):
        at = pl.multiple_of(part * ff + k * SILU_BLOCK, SILU_BLOCK)
        return pltpu.make_async_copy(
            rest.at[:, pl.ds(at, SILU_BLOCK)],
            gates.at[k, :, part * SILU_BLOCK : (part + 1) * SILU_BLOCK],
            gate_sems.at[k, part],
        )

    def bring_down(k):
        at = pl.ds(pl.multiple_of(k * step, step), step)
        return (
            pltpu.make_async_copy(resid_hbm.at[:, at], resid.at[:, at], down_sems.at[k, 0]),
            pltpu.make_async_copy(
                rest.at[at, 2 * ff : 3 * ff], downs.at[at], down_sems.at[k, 1]
            ),
        )

    quarter = depth // QUARTERS

    def bring_first(q):
        at = slice(q * quarter, (q + 1) * quarter)
        return (
            pltpu.make_async_copy(normed_hbm.at[:, at], normed.at[:, at], first_sems.at[q, 0]),
            pltpu.make_async_copy(
                rest.at[at, :SILU_BLOCK], gates.at[0, at, :SILU_BLOCK], first_sems.at[q, 1]
            ),
            pltpu.make_async_copy(
                rest.at[at, ff : ff + SILU_BLOCK],
                gates.at[0, at, SILU_BLOCK:],
                first_sems.at[q, 2],
            ),
        )

    def start_down(k, carry):
        for copy in bring_down(k):
            copy.start()
        return carry

    def start_gate(k):
        bring_gate(k, 0).start()
        bring_gate(k, 1).start()

    def hide(k, both):
        gate = both[:, :SILU_BLOCK]
        hidden[:, pl.ds(pl.multiple_of(k * SILU_BLOCK, SILU_BLOCK), SILU_BLOCK)] = (
            gate / (1.0 + jnp.exp(-gate)) * both[:, SILU_BLOCK:]
        ).astype(jnp.bfloat16)

    for q in range(QUARTERS):
        for copy in bring_first(q):
            copy.start()
    both = 0.0
    for q in range(QUARTERS):
        for copy in bring_first(q):
            copy.wait()
        if q == QUARTERS // 2:
            start_gate(1)
        if q == QUARTERS - 1:
            start_gate(2)
        at = slice(q * quarter, (q + 1) * quarter)
        both += jnp.dot(normed[:, at], gates[0, at], preferred_element_type=jnp.float32)
    hide(0, both)

    def one_gate(k, carry):
        bring_gate(k, 0).wait()
        bring_gate(k, 1).wait()

        @pl.when(k + 2 < blocks)
        def _():
            start_gate(k + 2)

        @pl.when(k >= blocks - 2)
        def _():
            share = last // 2
            begin = (k - blocks + 2) * share
            lax.fori_loop(begin, begin + share, start_down, 0)

        hide(k, jnp.dot(normed[...], gates[k], preferred_element_type=jnp.float32))
        return carry

    lax.fori_loop(1, blocks, one_gate, 0)

    def leave(k, slot):
        at = pl.ds(pl.multiple_of(k * step, step), step)
        return pltpu.make_async_copy(staged.at[slot], mixed.at[:, at], stage_sems.at[slot])

    def add_hidden(k, carry):
        slot = lax.rem(k, 2)
        at = pl.ds(pl.multiple_of(k * step, step), step)
        for copy in bring_down(k):
            copy.wait()
        product = lax.dot_general(hidden[...], downs[at, :], nt, preferred_element_type=jnp.float32)

        @pl.when(k >= 2)
        def _():
            leave(k - 2, slot).wait()

        staged[slot] = (resid[:, at].astype(jnp.float32) + product).astype(jnp.bfloat16)
        leave(k, slot).start()
        return carry

    lax.fori_loop(0, last, add_hidden, 0)
    leave(last - 2, 0).wait()
    leave(last - 1, 1).wait()


def mlp(resid, normed, rest, ff):
    rows, depth = resid.shape
    blocks = ff // SILU_BLOCK
    bf16 = jnp.bfloat16
    return pl.pallas_call(
        mlp_kernel,
        out_shape=jax.ShapeDtypeStruct((rows, depth), bf16),
        in_specs=[HBM, HBM, HBM],
        out_specs=HBM,
        scratch_shapes=[
            pltpu.VMEM((rows, depth), bf16),
            pltpu.VMEM((rows, depth), bf16),
            pltpu.VMEM((blocks, depth, 2 * SILU_BLOCK), bf16),
            pltpu.VMEM((depth, ff), bf16),
            pltpu.VMEM((rows, ff), bf16),
            pltpu.VMEM((2, rows, 512), bf16),
            pltpu.SemaphoreType.DMA((QUARTERS, 3)),
            pltpu.SemaphoreType.DMA((blocks, 2)),
            pltpu.SemaphoreType.DMA((depth // 512, 2)),
            pltpu.SemaphoreType.DMA((2,)),
        ],
        compiler_params=pltpu.CompilerParams(vmem_limit_bytes=60 << 20),
        cost_estimate=pl.CostEstimate(
            flops=6 * rows * depth * ff,
            bytes_accessed=6 * depth * ff,
            transcendentals=rows * ff,
        ),
        name="mlp",
    )(resid, normed, rest)


def per_device(
    tokens, doc_ids, attn_gain, mlp_gain, w_query, w_key_value, w_out, w_gate, w_up, w_down
):
    rows = tokens.shape[0]
    rank = lax.axis_index(RANKS)
    ff = w_gate.shape[1]
    unit = w_gate.shape[0]
    rest = lax.all_gather(
        jnp.concatenate([w_gate, w_up, w_down.T], axis=1), RANKS, axis=0, tiled=True
    )

    query_width = w_query.shape[1]
    pair_width = w_key_value.shape[1]
    head = pair_width // 2
    normed = rms_scale(tokens, attn_gain)
    position = rank * rows + jnp.arange(rows, dtype=jnp.int32)
    freqs = THETA ** (-2.0 * jnp.arange(head // 2, dtype=jnp.float32) / head)
    angle = position.astype(jnp.float32)[:, None] * freqs[None, :]
    cosine = jnp.cos(angle)
    sine = jnp.sin(angle)
    cosine, sine = (
        jnp.concatenate([cosine, cosine], axis=1),
        jnp.concatenate([-sine, sine], axis=1),
    )
    marks = doc_ids + 1
    mark_rows = jnp.pad(
        marks.astype(jnp.bfloat16).reshape(-1, pair_width),
        ((0, MARK_ROWS - rows // pair_width), (0, 0)),
    )
    coords = jnp.stack([lax.axis_index(name) for name in ("x", "y", "z", "core")]).astype(jnp.int32)

    both = query_width + pair_width
    queries, pairs = gathered(
        jnp.concatenate([w_query, w_key_value], axis=1), "x", (0, query_width, both)
    )
    (pairs,) = gathered(pairs, "y", (0, pair_width))
    (queries,) = gathered(queries, "z", (0, query_width))
    outs = w_out.T
    (outs,) = gathered(outs, "y", (0, outs.shape[1]))
    (outs,) = gathered(outs, "z", (0, outs.shape[1]))
    pair_first = first_step(pairs, "z")
    pair_first, cosine, sine, mark_rows, coords = lax.optimization_barrier(
        (pair_first, cosine, sine, mark_rows, coords)
    )
    pair_pieces = second_step(*pair_first, "z")
    query_pieces = second_step(*first_step(queries, "y"), "y")
    out_pieces = second_step(*first_step(outs, "x"), "x")
    sent = project(
        project_pairs_kernel,
        coords,
        [normed, cosine, sine, mark_rows],
        pair_pieces,
        unit,
        rows + MARK_ROWS,
    )
    halos = [shifted(sent, RANKS, by) for by in range(1, SPAN + 1)]
    query = project(project_query_kernel, coords, [normed, cosine, sine], query_pieces, unit, rows)
    attended = attend(query, marks.astype(jnp.float32)[None, :], [sent] + halos)
    resid, normed_mlp = add_out(coords, attended, mlp_gain[None, :], tokens, out_pieces, unit)
    return mlp(resid, normed_mlp, rest, ff)


def solution(mesh):
    chips = Mesh(mesh.devices.reshape(RING, RING, 2, RING), RANKS)
    in_specs = (
        P(RANKS, None),
        P(RANKS),
        P(),
        P(),
        P(RANKS, None),
        P(RANKS, None),
        P(None, RANKS),
        P(RANKS, None),
        P(RANKS, None),
        P(None, RANKS),
    )
    out_specs = P(RANKS, None)
    return jax.shard_map(
        per_device, mesh=chips, in_specs=in_specs, out_specs=out_specs, check_vma=False
    )
```

```python
import functools
import math

import jax
import jax.numpy as jnp
from jax import lax
from jax.experimental import pallas as pl
from jax.experimental.pallas import tpu as pltpu
from jax.sharding import Mesh
from jax.sharding import PartitionSpec as P

SPAN = 4


EPS = 1e-05
THETA = 500000.0
NEGATIVE = -1e30
RANKS = ("y", "z", "core", "x")
RING = 4
DELTAS = (0, -1, 1, 2)
MARK_ROWS = 16
SILU_BLOCK = 256
QUARTERS = 4


VMEM = pl.BlockSpec(memory_space=pltpu.VMEM)
SMEM = pl.BlockSpec(memory_space=pltpu.SMEM)
HBM = pl.BlockSpec(memory_space=pl.ANY)


def shifted(array, axis, by):
    length = lax.axis_size(axis)
    pairs = [(i, i + by) for i in range(length) if 0 <= i + by < length]
    return lax.ppermute(array, axis, pairs)


def turned(array, axis, by):
    return lax.ppermute(array, axis, [(i, (i + by) % RING) for i in range(RING)])


def rms_scale(values, gain):
    wide = values.astype(jnp.float32)
    power = jnp.mean(wide * wide, axis=-1, keepdims=True)
    return (wide * lax.rsqrt(power + EPS) * gain).astype(jnp.bfloat16)


def attend_kernel(head, query, marks, *refs):
    blocks = refs[:-4]
    attended, bias, scores, weights = refs[-4:]
    rows = query.shape[0]
    tile = 128
    per_row = blocks[0].shape[1] // tile
    for k, block in enumerate(blocks):
        for part in range(rows // tile):
            line = block[rows + part // per_row : rows + part // per_row + 1, :].astype(jnp.float32)
            line = line[:, (part % per_row) * tile : (part % per_row + 1) * tile]
            column = jnp.transpose(jnp.broadcast_to(line, (tile, tile)))
            for lane in range(rows // tile):
                same = column == marks[:, lane * tile : (lane + 1) * tile]
                if k == 0:
                    key = lax.broadcasted_iota(jnp.int32, (tile, tile), 0) + part * tile
                    place = lax.broadcasted_iota(jnp.int32, (tile, tile), 1) + lane * tile
                    same = same & (key <= place)
                bias[
                    k * rows + part * tile : k * rows + (part + 1) * tile,
                    lane * tile : (lane + 1) * tile,
                ] = jnp.where(same, 0.0, NEGATIVE)
    factor = 1.0 / math.sqrt(head)

    def one_head(h, carry):
        at = pl.ds(pl.multiple_of(h * head, head), head)
        peak = jnp.full((1, rows), NEGATIVE, jnp.float32)
        for k, block in enumerate(blocks):
            raw = lax.dot_general(
                block[:rows, :head],
                query[:, at],
                (((1,), (1,)), ((), ())),
                preferred_element_type=jnp.float32,
            )
            raw = raw * factor + bias[k * rows : (k + 1) * rows, :]
            scores[k * rows : (k + 1) * rows, :] = raw
            peak = jnp.maximum(peak, jnp.max(raw, axis=0, keepdims=True))
        totals = jnp.zeros((1, rows), jnp.float32)
        mixed = jnp.zeros((head, rows), jnp.float32)
        for k, block in enumerate(blocks):
            weight = jnp.exp(scores[k * rows : (k + 1) * rows, :] - peak)
            totals += jnp.sum(weight, axis=0, keepdims=True)
            weights[...] = weight.astype(jnp.bfloat16)
            mixed += lax.dot_general(
                block[:rows, head:],
                weights[...],
                (((0,), (0,)), ((), ())),
                preferred_element_type=jnp.float32,
            )
        attended[:, at] = jnp.transpose(mixed / totals).astype(jnp.bfloat16)
        return carry

    lax.fori_loop(0, query.shape[1] // head, one_head, 0)


def attend(query, marks, blocks):
    rows, width = query.shape
    head = blocks[0].shape[1] // 2
    keys = rows * len(blocks)
    vmem = pl.BlockSpec(memory_space=pltpu.VMEM)
    return pl.pallas_call(
        functools.partial(attend_kernel, head),
        out_shape=jax.ShapeDtypeStruct((rows, width), jnp.bfloat16),
        in_specs=[vmem] * (2 + len(blocks)),
        out_specs=vmem,
        scratch_shapes=[
            pltpu.VMEM((keys, rows), jnp.float32),
            pltpu.VMEM((keys, rows), jnp.float32),
            pltpu.VMEM((rows, rows), jnp.bfloat16),
        ],
        compiler_params=pltpu.CompilerParams(vmem_limit_bytes=32 << 20),
        cost_estimate=pl.CostEstimate(
            flops=4 * rows * keys * width,
            bytes_accessed=4 * rows * width + 4 * keys * head,
            transcendentals=keys * rows * (width // head),
        ),
        name="attend",
    )(query, marks, *blocks)


def place_kernel(splits, me, *refs):
    pieces, outs = refs[:RING], refs[RING:]
    rows = pieces[0].shape[0]
    for k, piece in enumerate(pieces):
        at = pl.ds(pl.multiple_of(lax.rem(me[0] + k, RING) * rows, rows), rows)
        for out, begin, end in zip(outs, splits, splits[1:]):
            out[at, :] = piece[:, begin:end]


def gathered(block, axis, splits):
    pieces = [block] + [turned(block, axis, -k) for k in range(1, RING)]
    rows = block.shape[0]
    return pl.pallas_call(
        functools.partial(place_kernel, splits),
        out_shape=tuple(
            jax.ShapeDtypeStruct((RING * rows, end - begin), block.dtype)
            for begin, end in zip(splits, splits[1:])
        ),
        in_specs=[SMEM] + [VMEM] * RING,
        out_specs=tuple(VMEM for _ in splits[1:]),
        compiler_params=pltpu.CompilerParams(vmem_limit_bytes=8 << 20),
        cost_estimate=pl.CostEstimate(
            flops=RING * block.size, bytes_accessed=4 * RING * block.size, transcendentals=0
        ),
        name="place",
    )(lax.axis_index(axis).astype(jnp.int32)[None], *pieces)


def first_step(block, axis):
    return block, turned(block, axis, 1), turned(block, axis, -1)


def second_step(block, low, high, axis):
    half = block.shape[0] // 2
    far_low = turned(low[:half], axis, 1)
    far_high = turned(high[half:], axis, -1)
    pieces = (block, low, high, far_low, far_high)
    swap = [(0, 1), (1, 0)]
    return pieces + tuple(lax.ppermute(piece, "core", swap) for piece in pieces)


def load_pieces(coords, pieces, order, target, sem, unit):
    count = len(pieces) // 2
    whole = order[0] == "x"
    line = RING * unit if whole else unit
    last = "xyz".index(order[2])

    def bring_line(second, first, begin):
        for swap in range(2):
            block, low, high, far_low, far_high = pieces[swap * count : (swap + 1) * count]
            owner = lax.rem(coords[3] + swap, 2)
            for outer in range(RING):
                came = {order[0]: first, order[1]: second}
                came[order[2]] = lax.rem(coords[last] + DELTAS[outer] + RING, RING)
                rank = ((came["y"] * RING + came["z"]) * 2 + owner) * RING + came["x"]
                piece = (block, low, high, (far_low, far_high)[begin])[outer]
                row = second * RING * unit + (0 if whole else first * unit)
                if outer == 3:
                    row = row - begin * 2 * RING * unit
                pltpu.make_async_copy(
                    piece.at[pl.ds(pl.multiple_of(row, unit), line)],
                    target.at[pl.ds(pl.multiple_of(rank * unit, unit), line)],
                    sem,
                ).start()

    for begin in range(2):
        if whole:
            for second in range(2 * begin, 2 * begin + 2):
                bring_line(second, 0, begin)
        else:

            def step(k, carry):
                bring_line(2 * begin + k // RING, lax.rem(k, RING), begin)
                return carry

            lax.fori_loop(0, 2 * RING, step, 0)


def rotated(raw, cosine, sine):
    return raw * cosine[...] + pltpu.roll(raw, raw.shape[1] // 2, 1) * sine[...]


def project_pairs_kernel(unit, coords, normed, cosine, sine, mark_rows, *refs):
    pieces = refs[:-3]
    pairs, weights, sem = refs[-3:]
    load_pieces(coords, pieces, "xyz", weights, sem, unit)
    rows = normed.shape[0]
    head = pairs.shape[1] // 2
    pairs[rows:, :] = mark_rows[...]
    pltpu.make_async_copy(weights, weights, sem).wait()
    raw = jnp.dot(normed[...], weights[...], preferred_element_type=jnp.float32)
    pairs[:rows, :head] = rotated(raw[:, :head], cosine, sine).astype(jnp.bfloat16)
    pairs[:rows, head:] = raw[:, head:].astype(jnp.bfloat16)


def project_query_kernel(unit, coords, normed, cosine, sine, *refs):
    pieces = refs[:-3]
    query, weights, sem = refs[-3:]
    head = cosine.shape[1]
    load_pieces(coords, pieces, "xzy", weights, sem, unit)
    pltpu.make_async_copy(weights, weights, sem).wait()
    raw = jnp.dot(normed[...], weights[...], preferred_element_type=jnp.float32)
    for begin in range(0, query.shape[1], head):
        query[:, begin : begin + head] = rotated(
            raw[:, begin : begin + head], cosine, sine
        ).astype(jnp.bfloat16)


def project(kernel, coords, held, pieces, unit, out_rows):
    rows, depth = held[0].shape
    width = pieces[0].shape[1]
    return pl.pallas_call(
        functools.partial(kernel, unit),
        out_shape=jax.ShapeDtypeStruct((out_rows, width), jnp.bfloat16),
        in_specs=[SMEM] + [VMEM] * len(held) + [HBM] * len(pieces),
        out_specs=VMEM,
        scratch_shapes=[
            pltpu.VMEM((depth, width), jnp.bfloat16),
            pltpu.SemaphoreType.DMA,
        ],
        compiler_params=pltpu.CompilerParams(vmem_limit_bytes=24 << 20),
        cost_estimate=pl.CostEstimate(
            flops=2 * rows * depth * width, bytes_accessed=2 * depth * width, transcendentals=0
        ),
    )(coords, *held, *pieces)


def out_kernel(unit, coords, attended, gain, tokens, *refs):
    pieces = refs[:10]
    resid_out, normed_out, held, outs, resid, normed, squares, token_sems, out_sem, leave_sems = refs[10:]
    _, depth = tokens.shape
    step = 1024
    last = depth // step
    nt = (((1,), (1,)), ((), ()))
    load_pieces(coords, pieces, "yzx", outs, out_sem, unit)

    def part(k):
        return pl.ds(pl.multiple_of(k * step, step), step)

    def bring(k):
        return pltpu.make_async_copy(tokens.at[:, part(k)], held.at[:, part(k)], token_sems.at[k])

    def leave(k, which):
        source, target = ((resid, resid_out), (normed, normed_out))[which]
        return pltpu.make_async_copy(
            source.at[:, part(k)], target.at[:, part(k)], leave_sems.at[k, which]
        )

    for k in range(last):
        bring(k).start()
    squares[...] = jnp.zeros_like(squares)
    pltpu.make_async_copy(outs, outs, out_sem).wait()

    def add_attended(k, carry):
        bring(k).wait()
        product = lax.dot_general(
            attended[...], outs[part(k), :], nt, preferred_element_type=jnp.float32
        )
        total = (held[:, part(k)].astype(jnp.float32) + product).astype(jnp.bfloat16)
        resid[:, part(k)] = total
        total = total.astype(jnp.float32)
        total = total * total
        squares[...] += sum(total[:, j * 128 : (j + 1) * 128] for j in range(step // 128))
        return carry

    lax.fori_loop(0, last, add_attended, 0)
    power = jnp.sum(squares[...], axis=1, keepdims=True) * (1.0 / depth)
    squares[...] = jnp.broadcast_to(lax.rsqrt(power + EPS), squares.shape)

    def scale(k, carry):
        leave(k, 0).start()
        for j in range(step // 128):
            at = pl.ds(pl.multiple_of(k * step + j * 128, 128), 128)
            normed[:, at] = (
                resid[:, at].astype(jnp.float32) * squares[...] * gain[:, at]
            ).astype(jnp.bfloat16)
        leave(k, 1).start()
        return carry

    lax.fori_loop(0, last, scale, 0)
    for k in range(last):
        leave(k, 0).wait()
        leave(k, 1).wait()


def add_out(coords, attended, gain, tokens, pieces, unit):
    rows, depth = tokens.shape
    key_width = attended.shape[1]
    whole = jax.ShapeDtypeStruct((rows, depth), jnp.bfloat16)
    held = pltpu.VMEM((rows, depth), jnp.bfloat16)
    return pl.pallas_call(
        functools.partial(out_kernel, unit),
        out_shape=(whole, whole),
        in_specs=[SMEM, VMEM, VMEM, HBM] + [HBM] * len(pieces),
        out_specs=(HBM, HBM),
        scratch_shapes=[
            held,
            pltpu.VMEM((depth, key_width), jnp.bfloat16),
            held,
            held,
            pltpu.VMEM((rows, 128), jnp.float32),
            pltpu.SemaphoreType.DMA((depth // 1024,)),
            pltpu.SemaphoreType.DMA,
            pltpu.SemaphoreType.DMA((depth // 1024, 2)),
        ],
        compiler_params=pltpu.CompilerParams(vmem_limit_bytes=56 << 20),
        cost_estimate=pl.CostEstimate(
            flops=2 * rows * depth * key_width,
            bytes_accessed=2 * depth * (key_width + 3 * rows),
            transcendentals=0,
        ),
        name="add_out",
    )(coords, attended, gain, tokens, *pieces)


def mlp_kernel(
    resid_hbm, normed_hbm, rest, mixed,
    resid, normed, gates, downs, hidden, staged,
    first_sems, gate_sems, down_sems, stage_sems,
):
    _, depth = resid.shape
    ff = hidden.shape[1]
    blocks = ff // SILU_BLOCK
    step = 1024
    last = depth // step
    nt = (((1,), (1,)), ((), ()))

    def bring_gate(k, part):
        at = pl.multiple_of(part * ff + k * SILU_BLOCK, SILU_BLOCK)
        return pltpu.make_async_copy(
            rest.at[:, pl.ds(at, SILU_BLOCK)],
            gates.at[k, :, part * SILU_BLOCK : (part + 1) * SILU_BLOCK],
            gate_sems.at[k, part],
        )

    def bring_down(k):
        at = pl.ds(pl.multiple_of(k * step, step), step)
        return (
            pltpu.make_async_copy(resid_hbm.at[:, at], resid.at[:, at], down_sems.at[k, 0]),
            pltpu.make_async_copy(
                rest.at[at, 2 * ff : 3 * ff], downs.at[at], down_sems.at[k, 1]
            ),
        )

    quarter = depth // QUARTERS

    def bring_first(q):
        at = slice(q * quarter, (q + 1) * quarter)
        return (
            pltpu.make_async_copy(normed_hbm.at[:, at], normed.at[:, at], first_sems.at[q, 0]),
            pltpu.make_async_copy(
                rest.at[at, :SILU_BLOCK], gates.at[0, at, :SILU_BLOCK], first_sems.at[q, 1]
            ),
            pltpu.make_async_copy(
                rest.at[at, ff : ff + SILU_BLOCK],
                gates.at[0, at, SILU_BLOCK:],
                first_sems.at[q, 2],
            ),
        )

    def start_down(k, carry):
        for copy in bring_down(k):
            copy.start()
        return carry

    def start_gate(k):
        bring_gate(k, 0).start()
        bring_gate(k, 1).start()

    def hide(k, both):
        gate = both[:, :SILU_BLOCK]
        hidden[:, pl.ds(pl.multiple_of(k * SILU_BLOCK, SILU_BLOCK), SILU_BLOCK)] = (
            gate / (1.0 + jnp.exp(-gate)) * both[:, SILU_BLOCK:]
        ).astype(jnp.bfloat16)

    for q in range(QUARTERS):
        for copy in bring_first(q):
            copy.start()
    both = 0.0
    for q in range(QUARTERS):
        for copy in bring_first(q):
            copy.wait()
        if q == QUARTERS // 2:
            start_gate(1)
        if q == QUARTERS - 1:
            start_gate(2)
        at = slice(q * quarter, (q + 1) * quarter)
        both += jnp.dot(normed[:, at], gates[0, at], preferred_element_type=jnp.float32)
    hide(0, both)

    def one_gate(k, carry):
        bring_gate(k, 0).wait()
        bring_gate(k, 1).wait()

        @pl.when(k + 2 < blocks)
        def _():
            start_gate(k + 2)

        @pl.when(k >= blocks - 2)
        def _():
            share = last // 2
            begin = (k - blocks + 2) * share
            lax.fori_loop(begin, begin + share, start_down, 0)

        hide(k, jnp.dot(normed[...], gates[k], preferred_element_type=jnp.float32))
        return carry

    lax.fori_loop(1, blocks, one_gate, 0)

    def leave(k, slot):
        at = pl.ds(pl.multiple_of(k * step, step), step)
        return pltpu.make_async_copy(staged.at[slot], mixed.at[:, at], stage_sems.at[slot])

    def add_hidden(k, carry):
        slot = lax.rem(k, 2)
        at = pl.ds(pl.multiple_of(k * step, step), step)
        for copy in bring_down(k):
            copy.wait()
        product = lax.dot_general(hidden[...], downs[at, :], nt, preferred_element_type=jnp.float32)

        @pl.when(k >= 2)
        def _():
            leave(k - 2, slot).wait()

        staged[slot] = (resid[:, at].astype(jnp.float32) + product).astype(jnp.bfloat16)
        leave(k, slot).start()
        return carry

    lax.fori_loop(0, last, add_hidden, 0)
    leave(last - 2, 0).wait()
    leave(last - 1, 1).wait()


def mlp(resid, normed, rest, ff):
    rows, depth = resid.shape
    blocks = ff // SILU_BLOCK
    bf16 = jnp.bfloat16
    return pl.pallas_call(
        mlp_kernel,
        out_shape=jax.ShapeDtypeStruct((rows, depth), bf16),
        in_specs=[HBM, HBM, HBM],
        out_specs=HBM,
        scratch_shapes=[
            pltpu.VMEM((rows, depth), bf16),
            pltpu.VMEM((rows, depth), bf16),
            pltpu.VMEM((blocks, depth, 2 * SILU_BLOCK), bf16),
            pltpu.VMEM((depth, ff), bf16),
            pltpu.VMEM((rows, ff), bf16),
            pltpu.VMEM((2, rows, 1024), bf16),
            pltpu.SemaphoreType.DMA((QUARTERS, 3)),
            pltpu.SemaphoreType.DMA((blocks, 2)),
            pltpu.SemaphoreType.DMA((depth // 512, 2)),
            pltpu.SemaphoreType.DMA((2,)),
        ],
        compiler_params=pltpu.CompilerParams(vmem_limit_bytes=60 << 20),
        cost_estimate=pl.CostEstimate(
            flops=6 * rows * depth * ff,
            bytes_accessed=6 * depth * ff,
            transcendentals=rows * ff,
        ),
        name="mlp",
    )(resid, normed, rest)


def per_device(
    tokens, doc_ids, attn_gain, mlp_gain, w_query, w_key_value, w_out, w_gate, w_up, w_down
):
    rows = tokens.shape[0]
    rank = lax.axis_index(RANKS)
    ff = w_gate.shape[1]
    unit = w_gate.shape[0]
    rest = lax.all_gather(
        jnp.concatenate([w_gate, w_up, w_down.T], axis=1), RANKS, axis=0, tiled=True
    )

    query_width = w_query.shape[1]
    pair_width = w_key_value.shape[1]
    head = pair_width // 2
    normed = rms_scale(tokens, attn_gain)
    position = rank * rows + jnp.arange(rows, dtype=jnp.int32)
    freqs = THETA ** (-2.0 * jnp.arange(head // 2, dtype=jnp.float32) / head)
    angle = position.astype(jnp.float32)[:, None] * freqs[None, :]
    cosine = jnp.cos(angle)
    sine = jnp.sin(angle)
    cosine, sine = (
        jnp.concatenate([cosine, cosine], axis=1),
        jnp.concatenate([-sine, sine], axis=1),
    )
    marks = doc_ids + 1
    mark_rows = jnp.pad(
        marks.astype(jnp.bfloat16).reshape(-1, pair_width),
        ((0, MARK_ROWS - rows // pair_width), (0, 0)),
    )
    coords = jnp.stack([lax.axis_index(name) for name in ("x", "y", "z", "core")]).astype(jnp.int32)

    both = query_width + pair_width
    queries, pairs = gathered(
        jnp.concatenate([w_query, w_key_value], axis=1), "x", (0, query_width, both)
    )
    (pairs,) = gathered(pairs, "y", (0, pair_width))
    (queries,) = gathered(queries, "z", (0, query_width))
    outs = w_out.T
    (outs,) = gathered(outs, "y", (0, outs.shape[1]))
    (outs,) = gathered(outs, "z", (0, outs.shape[1]))
    pair_first = first_step(pairs, "z")
    pair_first, cosine, sine, mark_rows, coords = lax.optimization_barrier(
        (pair_first, cosine, sine, mark_rows, coords)
    )
    pair_pieces = second_step(*pair_first, "z")
    query_pieces = second_step(*first_step(queries, "y"), "y")
    out_pieces = second_step(*first_step(outs, "x"), "x")
    sent = project(
        project_pairs_kernel,
        coords,
        [normed, cosine, sine, mark_rows],
        pair_pieces,
        unit,
        rows + MARK_ROWS,
    )
    halos = [shifted(sent, RANKS, by) for by in range(1, SPAN + 1)]
    query = project(project_query_kernel, coords, [normed, cosine, sine], query_pieces, unit, rows)
    attended = attend(query, marks.astype(jnp.float32)[None, :], [sent] + halos)
    resid, normed_mlp = add_out(coords, attended, mlp_gain[None, :], tokens, out_pieces, unit)
    return mlp(resid, normed_mlp, rest, ff)


def solution(mesh):
    chips = Mesh(mesh.devices.reshape(RING, RING, 2, RING), RANKS)
    in_specs = (
        P(RANKS, None),
        P(RANKS),
        P(),
        P(),
        P(RANKS, None),
        P(RANKS, None),
        P(None, RANKS),
        P(RANKS, None),
        P(RANKS, None),
        P(None, RANKS),
    )
    out_specs = P(RANKS, None)
    return jax.shard_map(
        per_device, mesh=chips, in_specs=in_specs, out_specs=out_specs, check_vma=False
    )
```

```python
import functools
import math

import jax
import jax.numpy as jnp
from jax import lax
from jax.experimental import pallas as pl
from jax.experimental.pallas import tpu as pltpu
from jax.sharding import Mesh
from jax.sharding import PartitionSpec as P

SPAN = 4


EPS = 1e-05
THETA = 500000.0
NEGATIVE = -1e30
RANKS = ("y", "z", "core", "x")
RING = 4
DELTAS = (0, -1, 1, 2)
MARK_ROWS = 16
SILU_BLOCK = 256
QUARTERS = 4


VMEM = pl.BlockSpec(memory_space=pltpu.VMEM)
SMEM = pl.BlockSpec(memory_space=pltpu.SMEM)
HBM = pl.BlockSpec(memory_space=pl.ANY)


def shifted(array, axis, by):
    length = lax.axis_size(axis)
    pairs = [(i, i + by) for i in range(length) if 0 <= i + by < length]
    return lax.ppermute(array, axis, pairs)


def turned(array, axis, by):
    return lax.ppermute(array, axis, [(i, (i + by) % RING) for i in range(RING)])


def rms_scale(values, gain):
    wide = values.astype(jnp.float32)
    power = jnp.mean(wide * wide, axis=-1, keepdims=True)
    return (wide * lax.rsqrt(power + EPS) * gain).astype(jnp.bfloat16)


def attend_kernel(head, query, marks, *refs):
    blocks = refs[:-4]
    attended, bias, scores, weights = refs[-4:]
    rows = query.shape[0]
    tile = 128
    per_row = blocks[0].shape[1] // tile
    for k, block in enumerate(blocks):
        for part in range(rows // tile):
            line = block[rows + part // per_row : rows + part // per_row + 1, :].astype(jnp.float32)
            line = line[:, (part % per_row) * tile : (part % per_row + 1) * tile]
            column = jnp.transpose(jnp.broadcast_to(line, (tile, tile)))
            for lane in range(rows // tile):
                same = column == marks[:, lane * tile : (lane + 1) * tile]
                if k == 0:
                    key = lax.broadcasted_iota(jnp.int32, (tile, tile), 0) + part * tile
                    place = lax.broadcasted_iota(jnp.int32, (tile, tile), 1) + lane * tile
                    same = same & (key <= place)
                bias[
                    k * rows + part * tile : k * rows + (part + 1) * tile,
                    lane * tile : (lane + 1) * tile,
                ] = jnp.where(same, 0.0, NEGATIVE)
    factor = 1.0 / math.sqrt(head)

    def one_head(h, carry):
        at = pl.ds(pl.multiple_of(h * head, head), head)
        peak = jnp.full((1, rows), NEGATIVE, jnp.float32)
        for k, block in enumerate(blocks):
            raw = lax.dot_general(
                block[:rows, :head],
                query[:, at],
                (((1,), (1,)), ((), ())),
                preferred_element_type=jnp.float32,
            )
            raw = raw * factor + bias[k * rows : (k + 1) * rows, :]
            scores[k * rows : (k + 1) * rows, :] = raw
            peak = jnp.maximum(peak, jnp.max(raw, axis=0, keepdims=True))
        totals = jnp.zeros((1, rows), jnp.float32)
        mixed = jnp.zeros((head, rows), jnp.float32)
        for k, block in enumerate(blocks):
            weight = jnp.exp(scores[k * rows : (k + 1) * rows, :] - peak)
            totals += jnp.sum(weight, axis=0, keepdims=True)
            weights[...] = weight.astype(jnp.bfloat16)
            mixed += lax.dot_general(
                block[:rows, head:],
                weights[...],
                (((0,), (0,)), ((), ())),
                preferred_element_type=jnp.float32,
            )
        attended[:, at] = jnp.transpose(mixed / totals).astype(jnp.bfloat16)
        return carry

    lax.fori_loop(0, query.shape[1] // head, one_head, 0)


def attend(query, marks, blocks):
    rows, width = query.shape
    head = blocks[0].shape[1] // 2
    keys = rows * len(blocks)
    vmem = pl.BlockSpec(memory_space=pltpu.VMEM)
    return pl.pallas_call(
        functools.partial(attend_kernel, head),
        out_shape=jax.ShapeDtypeStruct((rows, width), jnp.bfloat16),
        in_specs=[vmem] * (2 + len(blocks)),
        out_specs=vmem,
        scratch_shapes=[
            pltpu.VMEM((keys, rows), jnp.float32),
            pltpu.VMEM((keys, rows), jnp.float32),
            pltpu.VMEM((rows, rows), jnp.bfloat16),
        ],
        compiler_params=pltpu.CompilerParams(vmem_limit_bytes=32 << 20),
        cost_estimate=pl.CostEstimate(
            flops=4 * rows * keys * width,
            bytes_accessed=4 * rows * width + 4 * keys * head,
            transcendentals=keys * rows * (width // head),
        ),
        name="attend",
    )(query, marks, *blocks)


def place_kernel(splits, me, *refs):
    pieces, outs = refs[:RING], refs[RING:]
    rows = pieces[0].shape[0]
    for k, piece in enumerate(pieces):
        at = pl.ds(pl.multiple_of(lax.rem(me[0] + k, RING) * rows, rows), rows)
        for out, begin, end in zip(outs, splits, splits[1:]):
            out[at, :] = piece[:, begin:end]


def gathered(block, axis, splits):
    pieces = [block] + [turned(block, axis, -k) for k in range(1, RING)]
    rows = block.shape[0]
    return pl.pallas_call(
        functools.partial(place_kernel, splits),
        out_shape=tuple(
            jax.ShapeDtypeStruct((RING * rows, end - begin), block.dtype)
            for begin, end in zip(splits, splits[1:])
        ),
        in_specs=[SMEM] + [VMEM] * RING,
        out_specs=tuple(VMEM for _ in splits[1:]),
        compiler_params=pltpu.CompilerParams(vmem_limit_bytes=8 << 20),
        cost_estimate=pl.CostEstimate(
            flops=RING * block.size, bytes_accessed=4 * RING * block.size, transcendentals=0
        ),
        name="place",
    )(lax.axis_index(axis).astype(jnp.int32)[None], *pieces)


def first_step(block, axis):
    return block, turned(block, axis, 1), turned(block, axis, -1)


def second_step(block, low, high, axis):
    half = block.shape[0] // 2
    far_low = turned(low[:half], axis, 1)
    far_high = turned(high[half:], axis, -1)
    pieces = (block, low, high, far_low, far_high)
    swap = [(0, 1), (1, 0)]
    return pieces + tuple(lax.ppermute(piece, "core", swap) for piece in pieces)


def load_pieces(coords, pieces, order, target, sem, unit):
    count = len(pieces) // 2
    whole = order[0] == "x"
    line = RING * unit if whole else unit
    last = "xyz".index(order[2])

    def bring_line(second, first, begin):
        for swap in range(2):
            block, low, high, far_low, far_high = pieces[swap * count : (swap + 1) * count]
            owner = lax.rem(coords[3] + swap, 2)
            for outer in range(RING):
                came = {order[0]: first, order[1]: second}
                came[order[2]] = lax.rem(coords[last] + DELTAS[outer] + RING, RING)
                rank = ((came["y"] * RING + came["z"]) * 2 + owner) * RING + came["x"]
                piece = (block, low, high, (far_low, far_high)[begin])[outer]
                row = second * RING * unit + (0 if whole else first * unit)
                if outer == 3:
                    row = row - begin * 2 * RING * unit
                pltpu.make_async_copy(
                    piece.at[pl.ds(pl.multiple_of(row, unit), line)],
                    target.at[pl.ds(pl.multiple_of(rank * unit, unit), line)],
                    sem,
                ).start()

    for begin in range(2):
        if whole:
            for second in range(2 * begin, 2 * begin + 2):
                bring_line(second, 0, begin)
        else:

            def step(k, carry):
                bring_line(2 * begin + k // RING, lax.rem(k, RING), begin)
                return carry

            lax.fori_loop(0, 2 * RING, step, 0)


def rotated(raw, cosine, sine):
    return raw * cosine[...] + pltpu.roll(raw, raw.shape[1] // 2, 1) * sine[...]


def project_pairs_kernel(unit, coords, normed, cosine, sine, mark_rows, *refs):
    pieces = refs[:-3]
    pairs, weights, sem = refs[-3:]
    load_pieces(coords, pieces, "yzx", weights, sem, unit)
    rows = normed.shape[0]
    head = pairs.shape[1] // 2
    pairs[rows:, :] = mark_rows[...]
    pltpu.make_async_copy(weights, weights, sem).wait()
    raw = jnp.dot(normed[...], weights[...], preferred_element_type=jnp.float32)
    pairs[:rows, :head] = rotated(raw[:, :head], cosine, sine).astype(jnp.bfloat16)
    pairs[:rows, head:] = raw[:, head:].astype(jnp.bfloat16)


def project_query_kernel(unit, coords, normed, cosine, sine, *refs):
    pieces = refs[:-3]
    query, weights, sem = refs[-3:]
    head = cosine.shape[1]
    load_pieces(coords, pieces, "xzy", weights, sem, unit)
    pltpu.make_async_copy(weights, weights, sem).wait()
    raw = jnp.dot(normed[...], weights[...], preferred_element_type=jnp.float32)
    for begin in range(0, query.shape[1], head):
        query[:, begin : begin + head] = rotated(
            raw[:, begin : begin + head], cosine, sine
        ).astype(jnp.bfloat16)


def project(kernel, coords, held, pieces, unit, out_rows):
    rows, depth = held[0].shape
    width = pieces[0].shape[1]
    return pl.pallas_call(
        functools.partial(kernel, unit),
        out_shape=jax.ShapeDtypeStruct((out_rows, width), jnp.bfloat16),
        in_specs=[SMEM] + [VMEM] * len(held) + [HBM] * len(pieces),
        out_specs=VMEM,
        scratch_shapes=[
            pltpu.VMEM((depth, width), jnp.bfloat16),
            pltpu.SemaphoreType.DMA,
        ],
        compiler_params=pltpu.CompilerParams(vmem_limit_bytes=24 << 20),
        cost_estimate=pl.CostEstimate(
            flops=2 * rows * depth * width, bytes_accessed=2 * depth * width, transcendentals=0
        ),
    )(coords, *held, *pieces)


def out_kernel(unit, coords, attended, gain, tokens, *refs):
    pieces = refs[:10]
    resid_out, normed_out, held, outs, resid, normed, squares, token_sems, out_sem, leave_sems = refs[10:]
    _, depth = tokens.shape
    step = 1024
    last = depth // step
    nt = (((1,), (1,)), ((), ()))
    load_pieces(coords, pieces, "xyz", outs, out_sem, unit)

    def part(k):
        return pl.ds(pl.multiple_of(k * step, step), step)

    def bring(k):
        return pltpu.make_async_copy(tokens.at[:, part(k)], held.at[:, part(k)], token_sems.at[k])

    def leave(k, which):
        source, target = ((resid, resid_out), (normed, normed_out))[which]
        return pltpu.make_async_copy(
            source.at[:, part(k)], target.at[:, part(k)], leave_sems.at[k, which]
        )

    for k in range(last):
        bring(k).start()
    squares[...] = jnp.zeros_like(squares)
    pltpu.make_async_copy(outs, outs, out_sem).wait()

    def add_attended(k, carry):
        bring(k).wait()
        product = lax.dot_general(
            attended[...], outs[part(k), :], nt, preferred_element_type=jnp.float32
        )
        total = (held[:, part(k)].astype(jnp.float32) + product).astype(jnp.bfloat16)
        resid[:, part(k)] = total
        total = total.astype(jnp.float32)
        total = total * total
        squares[...] += sum(total[:, j * 128 : (j + 1) * 128] for j in range(step // 128))
        return carry

    lax.fori_loop(0, last, add_attended, 0)
    power = jnp.sum(squares[...], axis=1, keepdims=True) * (1.0 / depth)
    squares[...] = jnp.broadcast_to(lax.rsqrt(power + EPS), squares.shape)

    def scale(k, carry):
        leave(k, 0).start()
        for j in range(step // 128):
            at = pl.ds(pl.multiple_of(k * step + j * 128, 128), 128)
            normed[:, at] = (
                resid[:, at].astype(jnp.float32) * squares[...] * gain[:, at]
            ).astype(jnp.bfloat16)
        leave(k, 1).start()
        return carry

    lax.fori_loop(0, last, scale, 0)
    for k in range(last):
        leave(k, 0).wait()
        leave(k, 1).wait()


def add_out(coords, attended, gain, tokens, pieces, unit):
    rows, depth = tokens.shape
    key_width = attended.shape[1]
    whole = jax.ShapeDtypeStruct((rows, depth), jnp.bfloat16)
    held = pltpu.VMEM((rows, depth), jnp.bfloat16)
    return pl.pallas_call(
        functools.partial(out_kernel, unit),
        out_shape=(whole, whole),
        in_specs=[SMEM, VMEM, VMEM, HBM] + [HBM] * len(pieces),
        out_specs=(HBM, HBM),
        scratch_shapes=[
            held,
            pltpu.VMEM((depth, key_width), jnp.bfloat16),
            held,
            held,
            pltpu.VMEM((rows, 128), jnp.float32),
            pltpu.SemaphoreType.DMA((depth // 1024,)),
            pltpu.SemaphoreType.DMA,
            pltpu.SemaphoreType.DMA((depth // 1024, 2)),
        ],
        compiler_params=pltpu.CompilerParams(vmem_limit_bytes=56 << 20),
        cost_estimate=pl.CostEstimate(
            flops=2 * rows * depth * key_width,
            bytes_accessed=2 * depth * (key_width + 3 * rows),
            transcendentals=0,
        ),
        name="add_out",
    )(coords, attended, gain, tokens, *pieces)


def mlp_kernel(
    resid_hbm, normed_hbm, rest, mixed,
    resid, normed, gates, downs, hidden, staged,
    first_sems, gate_sems, down_sems, stage_sems,
):
    _, depth = resid.shape
    ff = hidden.shape[1]
    blocks = ff // SILU_BLOCK
    step = 1024
    last = depth // step
    nt = (((1,), (1,)), ((), ()))

    def bring_gate(k, part):
        at = pl.multiple_of(part * ff + k * SILU_BLOCK, SILU_BLOCK)
        return pltpu.make_async_copy(
            rest.at[:, pl.ds(at, SILU_BLOCK)],
            gates.at[k, :, part * SILU_BLOCK : (part + 1) * SILU_BLOCK],
            gate_sems.at[k, part],
        )

    def bring_down(k):
        at = pl.ds(pl.multiple_of(k * step, step), step)
        return (
            pltpu.make_async_copy(resid_hbm.at[:, at], resid.at[:, at], down_sems.at[k, 0]),
            pltpu.make_async_copy(
                rest.at[at, 2 * ff : 3 * ff], downs.at[at], down_sems.at[k, 1]
            ),
        )

    quarter = depth // QUARTERS

    def bring_first(q):
        at = slice(q * quarter, (q + 1) * quarter)
        return (
            pltpu.make_async_copy(normed_hbm.at[:, at], normed.at[:, at], first_sems.at[q, 0]),
            pltpu.make_async_copy(
                rest.at[at, :SILU_BLOCK], gates.at[0, at, :SILU_BLOCK], first_sems.at[q, 1]
            ),
            pltpu.make_async_copy(
                rest.at[at, ff : ff + SILU_BLOCK],
                gates.at[0, at, SILU_BLOCK:],
                first_sems.at[q, 2],
            ),
        )

    def start_down(k, carry):
        for copy in bring_down(k):
            copy.start()
        return carry

    def start_gate(k):
        bring_gate(k, 0).start()
        bring_gate(k, 1).start()

    def hide(k, both):
        gate = both[:, :SILU_BLOCK]
        hidden[:, pl.ds(pl.multiple_of(k * SILU_BLOCK, SILU_BLOCK), SILU_BLOCK)] = (
            gate / (1.0 + jnp.exp(-gate)) * both[:, SILU_BLOCK:]
        ).astype(jnp.bfloat16)

    for q in range(QUARTERS):
        for copy in bring_first(q):
            copy.start()
    both = 0.0
    for q in range(QUARTERS):
        for copy in bring_first(q):
            copy.wait()
        if q == QUARTERS // 2:
            start_gate(1)
        if q == QUARTERS - 1:
            start_gate(2)
        at = slice(q * quarter, (q + 1) * quarter)
        both += jnp.dot(normed[:, at], gates[0, at], preferred_element_type=jnp.float32)
    hide(0, both)

    def one_gate(k, carry):
        bring_gate(k, 0).wait()
        bring_gate(k, 1).wait()

        @pl.when(k + 2 < blocks)
        def _():
            start_gate(k + 2)

        @pl.when(k >= blocks - 2)
        def _():
            share = last // 2
            begin = (k - blocks + 2) * share
            lax.fori_loop(begin, begin + share, start_down, 0)

        hide(k, jnp.dot(normed[...], gates[k], preferred_element_type=jnp.float32))
        return carry

    lax.fori_loop(1, blocks, one_gate, 0)

    def leave(k, slot):
        at = pl.ds(pl.multiple_of(k * step, step), step)
        return pltpu.make_async_copy(staged.at[slot], mixed.at[:, at], stage_sems.at[slot])

    def add_hidden(k, carry):
        slot = lax.rem(k, 2)
        at = pl.ds(pl.multiple_of(k * step, step), step)
        for copy in bring_down(k):
            copy.wait()
        product = lax.dot_general(hidden[...], downs[at, :], nt, preferred_element_type=jnp.float32)

        @pl.when(k >= 2)
        def _():
            leave(k - 2, slot).wait()

        staged[slot] = (resid[:, at].astype(jnp.float32) + product).astype(jnp.bfloat16)
        leave(k, slot).start()
        return carry

    lax.fori_loop(0, last, add_hidden, 0)
    leave(last - 2, 0).wait()
    leave(last - 1, 1).wait()


def mlp(resid, normed, rest, ff):
    rows, depth = resid.shape
    blocks = ff // SILU_BLOCK
    bf16 = jnp.bfloat16
    return pl.pallas_call(
        mlp_kernel,
        out_shape=jax.ShapeDtypeStruct((rows, depth), bf16),
        in_specs=[HBM, HBM, HBM],
        out_specs=HBM,
        scratch_shapes=[
            pltpu.VMEM((rows, depth), bf16),
            pltpu.VMEM((rows, depth), bf16),
            pltpu.VMEM((blocks, depth, 2 * SILU_BLOCK), bf16),
            pltpu.VMEM((depth, ff), bf16),
            pltpu.VMEM((rows, ff), bf16),
            pltpu.VMEM((2, rows, 1024), bf16),
            pltpu.SemaphoreType.DMA((QUARTERS, 3)),
            pltpu.SemaphoreType.DMA((blocks, 2)),
            pltpu.SemaphoreType.DMA((depth // 512, 2)),
            pltpu.SemaphoreType.DMA((2,)),
        ],
        compiler_params=pltpu.CompilerParams(vmem_limit_bytes=60 << 20),
        cost_estimate=pl.CostEstimate(
            flops=6 * rows * depth * ff,
            bytes_accessed=6 * depth * ff,
            transcendentals=rows * ff,
        ),
        name="mlp",
    )(resid, normed, rest)


def per_device(
    tokens, doc_ids, attn_gain, mlp_gain, w_query, w_key_value, w_out, w_gate, w_up, w_down
):
    rows = tokens.shape[0]
    rank = lax.axis_index(RANKS)
    ff = w_gate.shape[1]
    unit = w_gate.shape[0]
    rest = lax.all_gather(
        jnp.concatenate([w_gate, w_up, w_down.T], axis=1), RANKS, axis=0, tiled=True
    )

    query_width = w_query.shape[1]
    pair_width = w_key_value.shape[1]
    head = pair_width // 2
    normed = rms_scale(tokens, attn_gain)
    position = rank * rows + jnp.arange(rows, dtype=jnp.int32)
    freqs = THETA ** (-2.0 * jnp.arange(head // 2, dtype=jnp.float32) / head)
    angle = position.astype(jnp.float32)[:, None] * freqs[None, :]
    cosine = jnp.cos(angle)
    sine = jnp.sin(angle)
    cosine, sine = (
        jnp.concatenate([cosine, cosine], axis=1),
        jnp.concatenate([-sine, sine], axis=1),
    )
    marks = doc_ids + 1
    mark_rows = jnp.pad(
        marks.astype(jnp.bfloat16).reshape(-1, pair_width),
        ((0, MARK_ROWS - rows // pair_width), (0, 0)),
    )
    coords = jnp.stack([lax.axis_index(name) for name in ("x", "y", "z", "core")]).astype(jnp.int32)

    outs = w_out.T
    both = query_width + outs.shape[1]
    (pairs,) = gathered(w_key_value, "y", (0, pair_width))
    (pairs,) = gathered(pairs, "z", (0, pair_width))
    queries, outs = gathered(jnp.concatenate([w_query, outs], axis=1), "x", (0, query_width, both))
    (queries,) = gathered(queries, "z", (0, query_width))
    (outs,) = gathered(outs, "y", (0, both - query_width))
    pair_first = first_step(pairs, "x")
    pair_first, cosine, sine, mark_rows, coords = lax.optimization_barrier(
        (pair_first, cosine, sine, mark_rows, coords)
    )
    pair_pieces = second_step(*pair_first, "x")
    query_pieces = second_step(*first_step(queries, "y"), "y")
    out_pieces = second_step(*first_step(outs, "z"), "z")
    sent = project(
        project_pairs_kernel,
        coords,
        [normed, cosine, sine, mark_rows],
        pair_pieces,
        unit,
        rows + MARK_ROWS,
    )
    halos = [shifted(sent, RANKS, by) for by in range(1, SPAN + 1)]
    query = project(project_query_kernel, coords, [normed, cosine, sine], query_pieces, unit, rows)
    attended = attend(query, marks.astype(jnp.float32)[None, :], [sent] + halos)
    resid, normed_mlp = add_out(coords, attended, mlp_gain[None, :], tokens, out_pieces, unit)
    return mlp(resid, normed_mlp, rest, ff)


def solution(mesh):
    chips = Mesh(mesh.devices.reshape(RING, RING, 2, RING), RANKS)
    in_specs = (
        P(RANKS, None),
        P(RANKS),
        P(),
        P(),
        P(RANKS, None),
        P(RANKS, None),
        P(None, RANKS),
        P(RANKS, None),
        P(RANKS, None),
        P(None, RANKS),
    )
    out_specs = P(RANKS, None)
    return jax.shard_map(
        per_device, mesh=chips, in_specs=in_specs, out_specs=out_specs, check_vma=False
    )
```
